32 devices in a mesh: rep: 4 (over z), fsdp: 8 (over y, x, core).
Axes of the slice: x: 2, y: 2, z: 4, core: 2. Of those that a mesh axis runs over, the one named last changes fastest.
Arguments:
- tokens: bfloat16 [7680, 2048], P(('rep', 'fsdp')), may hold values from -6 to 6
- cotangent: bfloat16 [7680, 2048], P(('rep', 'fsdp')), may hold values from -6 to 6
- counts: int32 [4, 8, 8], P('rep'), may hold values from 24 to 36, as said below
- deal_order: int32 [4, 8], P('rep'), may hold values from 0 to 7, as said below
- seq_lengths: int32 [4, 8], P('rep', 'fsdp'), may hold values from 192 to 288, as said below
- input_gain: bfloat16 [2048], P('fsdp'), may hold values from 0.5 to 1.5
- w_query: bfloat16 [2048, 2048], P('fsdp'), may hold values from -0.125 to 0.125
- key_projection: bfloat16 [2048, 1024], P('fsdp'), may hold values from -0.125 to 0.125
- value_projection: bfloat16 [2048, 1024], P('fsdp'), may hold values from -0.125 to 0.125
- query_gain: bfloat16 [128], P('fsdp'), may hold values from 0.5 to 1.5
- key_gain: bfloat16 [128], P('fsdp'), may hold values from 0.5 to 1.5
- w_out: bfloat16 [2048, 2048], P('fsdp'), may hold values from -1 to 1
- mlp_gain: bfloat16 [2048], P('fsdp'), may hold values from 0.5 to 1.5
- w_gate: bfloat16 [2048, 6144], P('fsdp'), may hold values from -0.125 to 0.125
- w_up: bfloat16 [2048, 6144], P('fsdp'), may hold values from -0.125 to 0.125
- w_down: bfloat16 [6144, 2048], P('fsdp'), may hold values from -0.078125 to 0.078125
Outputs:
- output: bfloat16 [7680, 2048], P(('rep', 'fsdp'))
- input_grad: bfloat16 [7680, 2048], P(('rep', 'fsdp'))
- input_gain_grad: float32 [2048], P('fsdp')
- w_query_grad: float32 [2048, 2048], P('fsdp')
- w_key_grad: float32 [2048, 1024], P('fsdp')
- w_value_grad: float32 [2048, 1024], P('fsdp')
- query_gain_grad: float32 [128], P('fsdp')
- key_gain_grad: float32 [128], P('fsdp')
- w_out_grad: float32 [2048, 2048], P('fsdp')
- mlp_gain_grad: float32 [2048], P('fsdp')
- w_gate_grad: float32 [2048, 6144], P('fsdp')
- w_up_grad: float32 [2048, 6144], P('fsdp')
- w_down_grad: float32 [6144, 2048], P('fsdp')
The draws below stay inside these ranges and needn't reach their ends.
Inputs may be any that keep to these rules, and one draw needn't show every extreme that they name: Each device's counts over its runs sum to 240; every entry is 36 or 24; in each replica some run has 36 rows on every device. `deal_order`: each replica's row is a permutation of the devices. seq_lengths[r, deal_order[r, k]] equals the sum over f of counts[r, f, k], so no length is under 8 * 24; each replica has a sequence of 288 rows.
All inputs are finite; a program needn't handle non-finite values.
Results may differ from the reference program's by a relative error of at most 0.02.
Values may be sent and summed in bfloat16 or wider, within the bound.
A program may use at most 448 MiB of HBM per device.

```python
import jax
import jax.numpy as jnp
from jax import lax

MODEL_DIM = 2048
QUERY_HEADS = 16
KEY_VALUE_HEADS = 8
HEAD_SIZE = 128
FF = 6144
SLOT_LENGTH = 288
IN_ROWS = 240
TOKENS = 7680
N_REP = 4
N_FSDP = 8


def replica_tables(base_key):
    gathered_keys, pick_key, owner_key = jax.random.split(base_key, 3)
    groups = N_FSDP
    capacity = SLOT_LENGTH // groups
    reduce_by = SLOT_LENGTH // (3 * groups)
    full_run = jax.random.randint(gathered_keys, (), 0, groups)
    source_keys = jax.random.split(pick_key, groups)
    shuffles = jax.vmap(lambda one_key: jax.random.permutation(one_key, groups - 1))(source_keys)
    run_ids = jnp.arange(groups, dtype=jnp.int32)
    others = jnp.clip(jnp.where(run_ids < full_run, run_ids, run_ids - 1), 0, groups - 2)
    ranks_of = jnp.take(shuffles, others, axis=1)
    picked = (ranks_of < groups // 2) & (run_ids != full_run)[None, :]
    count_table = (capacity - reduce_by * picked.astype(jnp.int32)).astype(jnp.int32)
    run_owner = jax.random.permutation(owner_key, groups).astype(jnp.int32)
    run_lengths = jnp.sum(count_table, axis=0)
    inverse = jnp.argsort(run_owner, stable=True)
    lengths = jnp.take(run_lengths, inverse).astype(jnp.int32)
    return (count_table, run_owner, lengths)


def deal_tables(key):
    base = jax.random.fold_in(key, 4242)
    key_list = jax.random.split(base, N_REP)
    return jax.vmap(replica_tables)(key_list)


def draw_counts(key, part):
    return deal_tables(key)[0]


def draw_deal_order(key, part):
    return deal_tables(key)[1]


def draw_seq_lengths(key, part):
    return deal_tables(key)[2]


def shard_levels(rng, shape, cuts, low, top_value):
    def one(axis_at, shards_of):
        heights = jax.random.uniform(jax.random.fold_in(jax.random.fold_in(rng, 6), axis_at), (shards_of,), jnp.float32, low / len(cuts), top_value / len(cuts))
        return jnp.repeat(jnp.exp(heights), shape[axis_at] // shards_of).reshape((-1,) + (1,) * (len(shape) - axis_at - 1))

    gain = one(*cuts[0])
    for cut in cuts[1:]:
        gain = gain * one(*cut)
    return gain


def centred(stream_key, dims, spread, limit, pieces=(), kind=jnp.bfloat16):
    drawn = jax.random.normal(stream_key, dims, jnp.float32) * spread
    if len(pieces) > 0:
        drawn = shard_levels(stream_key, dims, pieces, -0.22, 0.18) * drawn
    return jnp.clip(drawn, min=-limit, max=limit).astype(kind)


def setup_inputs(seed: int = 0) -> dict:
    arg_keys = jax.random.split(jax.random.key(seed), 17)
    return {
        "tokens": centred(arg_keys[0], (TOKENS, MODEL_DIM), 1.0, 6.0, ((0, 32),)),
        "cotangent": centred(arg_keys[1], (TOKENS, MODEL_DIM), 1.0, 6.0, ((0, 32),)),
        "counts": draw_counts(jax.random.fold_in(arg_keys[16], 71), 0),
        "deal_order": draw_deal_order(jax.random.fold_in(arg_keys[16], 71), 0),
        "seq_lengths": draw_seq_lengths(jax.random.fold_in(arg_keys[16], 71), 0),
        "input_gain": jnp.clip(1.0 + 0.1 * jax.random.normal(arg_keys[5], (MODEL_DIM,), jnp.float32), 0.5, 1.5).astype(jnp.bfloat16),
        "w_query": centred(arg_keys[6], (MODEL_DIM, QUERY_HEADS * HEAD_SIZE), MODEL_DIM ** -0.5, 0.125, ((0, 8),)),
        "key_projection": centred(arg_keys[7], (MODEL_DIM, KEY_VALUE_HEADS * HEAD_SIZE), MODEL_DIM ** -0.5, 0.125, ((0, 8),)),
        "value_projection": centred(arg_keys[8], (MODEL_DIM, KEY_VALUE_HEADS * HEAD_SIZE), MODEL_DIM ** -0.5, 0.125, ((0, 8),)),
        "query_gain": jnp.clip(1.0 + 0.1 * jax.random.normal(arg_keys[9], (HEAD_SIZE,), jnp.float32), 0.5, 1.5).astype(jnp.bfloat16),
        "key_gain": jnp.clip(1.0 + 0.1 * jax.random.normal(arg_keys[10], (HEAD_SIZE,), jnp.float32), 0.5, 1.5).astype(jnp.bfloat16),
        "w_out": centred(arg_keys[11], (QUERY_HEADS * HEAD_SIZE, MODEL_DIM), (QUERY_HEADS * HEAD_SIZE // 64) ** -0.5, 1.0, ((0, 8),)),
        "mlp_gain": jnp.clip(1.0 + 0.1 * jax.random.normal(arg_keys[12], (MODEL_DIM,), jnp.float32), 0.5, 1.5).astype(jnp.bfloat16),
        "w_gate": centred(arg_keys[13], (MODEL_DIM, FF), MODEL_DIM ** -0.5, 0.125, ((0, 8),)),
        "w_up": centred(arg_keys[14], (MODEL_DIM, FF), MODEL_DIM ** -0.5, 0.125, ((0, 8),)),
        "w_down": centred(arg_keys[15], (FF, MODEL_DIM), FF ** -0.5, 0.078125, ((0, 8),)),
    }


EPSILON = 1e-06
ROPE_BASE = 1000000.0
NEG_LARGE = -1e+30

@jax.custom_vjp
def lower_precision(v):
    return lax.optimization_barrier(v.astype(jnp.bfloat16)).astype(jnp.float32)

@jax.custom_vjp
def lower_precision_reverse(v):
    return v

def low_keep(v):
    return (lower_precision(v), None)

def low_pass(kept, grad):
    return (grad,)

def back_keep(v):
    return (v, None)

def back_low(kept, grad):
    return (lower_precision(grad),)
lower_precision.defvjp(low_keep, low_pass)
lower_precision_reverse.defvjp(back_keep, back_low)

def matrix_product(left, right):
    return jnp.dot(left, right, precision=lax.Precision.HIGHEST, preferred_element_type=jnp.float32)

def rms_scale(values):
    return lax.rsqrt(lax.optimization_barrier(jnp.mean(values * values, axis=-1, keepdims=True)) + EPSILON)

def rope_tables(sequence_length, head_width):
    positions = jnp.arange(sequence_length, dtype=jnp.float32)
    inverse = ROPE_BASE ** (-jnp.arange(0, head_width, 2, dtype=jnp.float32) / head_width)
    angles = positions[:, None] * inverse[None, :]
    angles = jnp.concatenate([angles, angles], axis=-1)
    return (jnp.cos(angles)[:, None, :], jnp.sin(angles)[:, None, :])

def rotate_half(values):
    halfway = values.shape[-1] // 2
    return jnp.concatenate([-values[..., halfway:], values[..., :halfway]], axis=-1)

def layer(params, row_block, seq_length):
    input_gain, w_query, key_projection, value_projection, query_gain, key_gain, w_out, mlp_gain, w_gate, w_up, w_down = params
    sequence_length = row_block.shape[0]
    attention_input = lower_precision(row_block * rms_scale(row_block) * input_gain)
    query_raw = lower_precision_reverse(matrix_product(attention_input, w_query)).reshape(sequence_length, QUERY_HEADS, HEAD_SIZE)
    key_unrotated = lower_precision_reverse(matrix_product(attention_input, key_projection)).reshape(sequence_length, KEY_VALUE_HEADS, HEAD_SIZE)
    value_reduced = lower_precision(lower_precision_reverse(matrix_product(attention_input, value_projection))).reshape(sequence_length, KEY_VALUE_HEADS, HEAD_SIZE)
    query_normed = query_raw * rms_scale(query_raw) * query_gain
    key_normed = key_unrotated * rms_scale(key_unrotated) * key_gain
    cosine_table, sine_table = rope_tables(sequence_length, HEAD_SIZE)
    query_rotated = lower_precision(query_normed * cosine_table + rotate_half(query_normed) * sine_table)
    key_rot = lower_precision(key_normed * cosine_table + rotate_half(key_normed) * sine_table)
    query_grouped = query_rotated.reshape(sequence_length, KEY_VALUE_HEADS, QUERY_HEADS // KEY_VALUE_HEADS, HEAD_SIZE)
    scores = jnp.einsum('ikgd,jkd->kgij', query_grouped, key_rot, precision=lax.Precision.HIGHEST) * HEAD_SIZE ** (-0.5)
    scores = lower_precision_reverse(scores)
    positions = jnp.arange(sequence_length, dtype=jnp.int32)
    visible = (positions[None, :] <= positions[:, None]) & (positions[None, :] < seq_length)
    scores = jnp.where(visible, scores, NEG_LARGE)
    attention = lower_precision(jax.nn.softmax(scores, axis=-1))
    context = jnp.einsum('kgij,jkd->ikgd', attention, value_reduced, precision=lax.Precision.HIGHEST)
    context = lower_precision(lower_precision_reverse(context.reshape(sequence_length, QUERY_HEADS * HEAD_SIZE)))
    hidden_one = row_block + lower_precision_reverse(matrix_product(context, w_out))
    mlp_in = lower_precision(hidden_one * rms_scale(hidden_one) * mlp_gain)
    gate_pre = lower_precision_reverse(matrix_product(mlp_in, w_gate))
    up_pre = lower_precision_reverse(matrix_product(mlp_in, w_up))
    activ = lower_precision(jax.nn.silu(gate_pre) * up_pre)
    return hidden_one + lower_precision_reverse(matrix_product(activ, w_down))

def reference(tokens, cotangent, counts, deal_order, seq_lengths, input_gain, w_query, key_projection, value_projection, query_gain, key_gain, w_out, mlp_gain, w_gate, w_up, w_down):
    groups = N_FSDP
    model_width = tokens.shape[1]
    total_rows = tokens.shape[0]
    positions = jnp.arange(SLOT_LENGTH, dtype=jnp.int32)
    run_start = jnp.cumsum(counts, axis=2) - counts
    column = jnp.transpose(counts, (0, 2, 1))
    column_start = jnp.cumsum(column, axis=2) - column
    column_end = column_start + column
    length_of = jnp.take_along_axis(seq_lengths, deal_order, axis=1).astype(jnp.int32)
    filled = jnp.minimum(lax.optimization_barrier(jnp.sum(column, axis=2)), length_of)
    source = lax.optimization_barrier(jnp.sum((column_end[:, :, None, :] <= positions[None, None, :, None]).astype(jnp.int32), axis=3))
    source = jnp.minimum(source, groups - 1).astype(jnp.int32)
    within = positions[None, None, :] - jnp.take_along_axis(column_start, source, axis=2)
    start_rows = jnp.take_along_axis(jnp.transpose(run_start, (0, 2, 1)), source, axis=2)
    replica = jnp.arange(N_REP, dtype=jnp.int32)[:, None, None]
    row_ids = (replica * groups + source) * IN_ROWS + start_rows + within
    is_live = positions[None, None, :] < filled[:, :, None]
    row_ids = jnp.where(is_live, row_ids, total_rows).astype(jnp.int32).reshape(-1)
    padded_in = jnp.concatenate([tokens.astype(jnp.float32), jnp.zeros((1, model_width), jnp.float32)], axis=0)
    padded_dy = jnp.concatenate([cotangent.astype(jnp.float32), jnp.zeros((1, model_width), jnp.float32)], axis=0)
    slots_in = jnp.take(padded_in, row_ids, axis=0).reshape(N_REP * groups, SLOT_LENGTH, model_width)
    slots_dy = jnp.take(padded_dy, row_ids, axis=0).reshape(N_REP * groups, SLOT_LENGTH, model_width)
    lengths = length_of.reshape(-1)
    params = tuple((weight.astype(jnp.float32) for weight in (input_gain, w_query, key_projection, value_projection, query_gain, key_gain, w_out, mlp_gain, w_gate, w_up, w_down)))

    def one_sequence(totals, sequence):
        row_block, grad_block, seq_length = sequence
        result, pullback = jax.vjp(lambda weights, inputs: layer(weights, inputs, seq_length), params, row_block)
        grad_params, grad_rows = pullback(grad_block)
        totals = jax.tree.map(lambda first, second: first + second, totals, grad_params)
        return (totals, (result, grad_rows))
    zero_totals = jax.tree.map(jnp.zeros_like, params)
    totals, (results, grad_rows) = lax.scan(one_sequence, zero_totals, (slots_in, slots_dy, lengths))
    local_ids = jnp.arange(IN_ROWS, dtype=jnp.int32)
    run_end = run_start + counts
    run_index = lax.optimization_barrier(jnp.sum((run_end[:, :, None, :] <= local_ids[None, None, :, None]).astype(jnp.int32), axis=3))
    run_index = jnp.minimum(run_index, groups - 1).astype(jnp.int32)
    inside = local_ids[None, None, :] - jnp.take_along_axis(run_start, run_index, axis=2)
    slot_pos = jnp.take_along_axis(jnp.transpose(column_start, (0, 2, 1)), run_index, axis=2) + inside
    filled_rf = jnp.take_along_axis(jnp.broadcast_to(filled[:, None, :], (N_REP, groups, groups)), run_index, axis=2)
    seq_index = replica * groups + run_index
    flat_index = jnp.where(slot_pos < filled_rf, seq_index * SLOT_LENGTH + slot_pos, N_REP * groups * SLOT_LENGTH).astype(jnp.int32).reshape(-1)
    padded_out = jnp.concatenate([results.reshape(-1, model_width), jnp.zeros((1, model_width), jnp.float32)], axis=0)
    padded_grad = jnp.concatenate([grad_rows.reshape(-1, model_width), jnp.zeros((1, model_width), jnp.float32)], axis=0)
    output = jnp.take(padded_out, flat_index, axis=0).astype(jnp.bfloat16)
    input_grad = jnp.take(padded_grad, flat_index, axis=0).astype(jnp.bfloat16)
    g_in, g_query, g_key, g_value, g_qgain, g_kgain, g_out, g_mlp, g_gate, g_up, g_down = totals
    return (output, input_grad, g_in, g_query, g_key, g_value, g_qgain, g_kgain, g_out, g_mlp, g_gate, g_up, g_down)
```

```python
import jax
import jax.numpy as jnp
from jax import lax
from jax.sharding import PartitionSpec as P

QUERY_HEADS = 16
KEY_VALUE_HEADS = 8
HEAD_SIZE = 128
SLOT_LENGTH = 288

EPSILON = 1e-06
ROPE_BASE = 1000000.0
NEG_LARGE = -1e30

F32 = jnp.float32
BF16 = jnp.bfloat16


def rms_scale(values):
    return lax.rsqrt(jnp.mean(values * values, axis=-1, keepdims=True) + EPSILON)


def dot(left, right):
    return jnp.dot(left, right, preferred_element_type=F32)


def dot_bt(left, right):
    return lax.dot_general(left, right, (((1,), (1,)), ((), ())), preferred_element_type=F32)


def dot_at(left, right):
    return lax.dot_general(left, right, (((0,), (0,)), ((), ())), preferred_element_type=F32)


def rotate_half(values):
    halfway = values.shape[-1] // 2
    return jnp.concatenate([-values[..., halfway:], values[..., :halfway]], axis=-1)


def rotate_back(values):
    halfway = values.shape[-1] // 2
    return jnp.concatenate([values[..., halfway:], -values[..., :halfway]], axis=-1)


def norm_back(grad_normed, unit_rows, scale_rows, gain_rows):
    scaled = grad_normed * gain_rows
    lead_axes = tuple(range(grad_normed.ndim - 1))
    grad_gain = jnp.sum(grad_normed * unit_rows, axis=lead_axes)
    grad_raw = scale_rows * (
        scaled - unit_rows * jnp.mean(scaled * unit_rows, axis=-1, keepdims=True)
    )
    return (grad_raw, grad_gain)


def pad_rows(values):
    return jnp.concatenate([values, jnp.zeros((1, values.shape[1]), values.dtype)], axis=0)


def on_device(
    tokens,
    cotangent,
    counts,
    deal_order,
    seq_lengths,
    input_gain,
    w_query,
    key_projection,
    value_projection,
    query_gain,
    key_gain,
    w_out,
    mlp_gain,
    w_gate,
    w_up,
    w_down,
):
    groups = lax.axis_size("fsdp")
    replicas = lax.axis_size("rep")
    device = lax.axis_index("fsdp")
    in_rows, width = tokens.shape
    cap = SLOT_LENGTH // groups
    shard = width // groups
    heads = QUERY_HEADS // groups
    kv_heads = max(1, KEY_VALUE_HEADS // groups)
    spread = max(1, groups // KEY_VALUE_HEADS)
    per_kv = heads // kv_heads
    q_cols, kv_cols = heads * HEAD_SIZE, kv_heads * HEAD_SIZE
    ff_cols = w_gate.shape[1] // groups

    def gather(values):
        return lax.all_gather(values, "fsdp", axis=0, tiled=True)

    def scatter_sum(values):
        return lax.psum_scatter(
            values.astype(BF16), "fsdp", scatter_dimension=0, tiled=True
        ).astype(F32)

    all_tokens = gather(tokens)
    gains = gather(jnp.concatenate([input_gain, mlp_gain, query_gain, key_gain])[None]).astype(F32)
    head_part = HEAD_SIZE // groups
    gain_one = gains[:, :shard].reshape(width)
    gain_two = gains[:, shard : 2 * shard].reshape(width)
    gain_query = gains[:, 2 * shard : 2 * shard + head_part].reshape(HEAD_SIZE)
    gain_key = gains[:, 2 * shard + head_part :].reshape(HEAD_SIZE)

    def kv_columns(weight):
        return jnp.repeat(
            weight.reshape(shard, KEY_VALUE_HEADS // kv_heads, kv_cols), spread, axis=1
        )

    send_attn = jnp.concatenate(
        [
            w_query.reshape(shard, groups, q_cols),
            kv_columns(key_projection),
            kv_columns(value_projection),
        ],
        axis=2,
    )
    w_qkv = lax.all_to_all(send_attn, "fsdp", split_axis=1, concat_axis=0, tiled=True).reshape(
        width, q_cols + 2 * kv_cols
    )
    send_ff = jnp.concatenate(
        [w_gate.reshape(shard, groups, ff_cols), w_up.reshape(shard, groups, ff_cols)], axis=2
    )
    w_ff = lax.all_to_all(send_ff, "fsdp", split_axis=1, concat_axis=0, tiled=True).reshape(
        width, 2 * ff_cols
    )
    all_grads = gather(cotangent)

    table = counts[0]
    run_start = jnp.cumsum(table, axis=1) - table
    seq_start = jnp.cumsum(table, axis=0) - table
    ids = jnp.arange(groups, dtype=jnp.int32)
    inner = jnp.arange(cap, dtype=jnp.int32)
    live = inner[None, None, :] < table.T[:, :, None]
    packed = ids[None, :, None] * in_rows + run_start.T[:, :, None] + inner[None, None, :]
    slot_index = jnp.where(live, packed, groups * in_rows).reshape(-1)
    place = (seq_start.T[:, :, None] + inner[None, None, :]).reshape(groups, SLOT_LENGTH)
    live = live.reshape(groups, SLOT_LENGTH)
    row_ids = jnp.arange(in_rows, dtype=jnp.int32)
    run_of = jnp.minimum(
        jnp.sum(((run_start + table)[:, None, :] <= row_ids[None, :, None]).astype(jnp.int32), 2),
        groups - 1,
    )
    run_hot = (run_of[:, :, None] == ids[None, None, :]).astype(jnp.int32)
    inside = row_ids[None, :] - jnp.sum(run_hot * run_start[:, None, :], axis=2)
    home_index = (run_of * SLOT_LENGTH + ids[:, None] * cap + inside).reshape(-1)

    def to_slots(values):
        return jnp.take(pad_rows(values), slot_index, axis=0)

    def to_packed(values):
        return jnp.take(values, home_index, axis=0)

    resid = tokens.astype(F32)
    scale_one = rms_scale(resid)
    normed_one = resid * scale_one
    all_resid = all_tokens.astype(F32)
    attention_input = (all_resid * rms_scale(all_resid) * gain_one).astype(BF16)
    raw = to_slots(dot(attention_input, w_qkv))
    query_raw = raw[:, :q_cols].reshape(groups, SLOT_LENGTH, heads, HEAD_SIZE)
    key_raw = raw[:, q_cols : q_cols + kv_cols].reshape(groups, SLOT_LENGTH, kv_heads, HEAD_SIZE)
    value = raw[:, q_cols + kv_cols :].astype(BF16).reshape(
        groups, SLOT_LENGTH, kv_heads, HEAD_SIZE
    )
    query_scale = rms_scale(query_raw)
    query_unit = query_raw * query_scale
    key_scale = rms_scale(key_raw)
    key_unit = key_raw * key_scale
    inverse = ROPE_BASE ** (-jnp.arange(0, HEAD_SIZE, 2, dtype=F32) / HEAD_SIZE)
    angles = place.astype(F32)[:, :, None] * inverse
    cosine = jnp.cos(angles)
    sine = jnp.sin(angles)
    cosine = jnp.concatenate([cosine, cosine], axis=-1)[:, :, None, :]
    sine = jnp.concatenate([sine, sine], axis=-1)[:, :, None, :]
    query_normed = query_unit * gain_query
    key_normed = key_unit * gain_key
    query = (query_normed * cosine + rotate_half(query_normed) * sine).astype(BF16)
    key = (key_normed * cosine + rotate_half(key_normed) * sine).astype(BF16)
    query = query.reshape(groups, SLOT_LENGTH, kv_heads, per_kv, HEAD_SIZE)
    visible = (place[:, None, :] <= place[:, :, None]) & live[:, None, :]
    visible = visible[:, None, None]
    softmax_scale = HEAD_SIZE ** (-0.5)
    scores = jnp.where(
        visible,
        jnp.einsum("sikgd,sjkd->skgij", query, key, preferred_element_type=F32) * softmax_scale,
        NEG_LARGE,
    )
    row_max = jnp.max(scores, axis=-1, keepdims=True)
    exp_scores = jnp.exp(scores - row_max)
    row_sum = jnp.sum(exp_scores, axis=-1, keepdims=True)
    probs = exp_scores / row_sum
    probs_low = probs.astype(BF16)
    context = jnp.einsum("skgij,sjkd->sikgd", probs_low, value, preferred_element_type=F32)
    context = to_packed(context.astype(BF16).reshape(groups * SLOT_LENGTH, q_cols))
    hidden_one = resid + scatter_sum(dot(context, w_out))

    scale_two = rms_scale(hidden_one)
    normed_two = hidden_one * scale_two
    mlp_in = gather((normed_two * gain_two).astype(BF16))
    gate_pre = dot(mlp_in, w_ff[:, :ff_cols])
    up_pre = dot(mlp_in, w_ff[:, ff_cols:])
    sigmoid_gate = jax.nn.sigmoid(gate_pre)
    activ = (gate_pre * sigmoid_gate * up_pre).astype(BF16)
    output = (hidden_one + scatter_sum(dot(activ, w_down))).astype(BF16)

    grad_activ = dot_bt(all_grads, w_down)
    grad_gate = (
        grad_activ * up_pre * sigmoid_gate * (1.0 + gate_pre * (1.0 - sigmoid_gate))
    ).astype(BF16)
    grad_up = (grad_activ * (gate_pre * sigmoid_gate)).astype(BF16)
    grad_ff = jnp.concatenate([grad_gate, grad_up], axis=1)
    down_term = dot_at(activ, all_grads).astype(BF16)
    ff_term = dot_at(mlp_in, grad_ff).astype(BF16)
    grad_mlp_in = scatter_sum(dot_bt(grad_ff, w_ff))
    grad_norm_two, gain_two_grad = norm_back(grad_mlp_in, normed_two, scale_two, gain_two)
    grad_hidden = cotangent.astype(F32) + grad_norm_two

    all_hidden = gather(grad_hidden.astype(BF16))
    out_term = dot_at(context, all_hidden).astype(BF16)
    grad_context = to_slots(dot_bt(all_hidden, w_out).astype(BF16)).reshape(
        groups, SLOT_LENGTH, kv_heads, per_kv, HEAD_SIZE
    )
    grad_probs = jnp.einsum("sikgd,sjkd->skgij", grad_context, value, preferred_element_type=F32)
    grad_value = jnp.einsum(
        "skgij,sikgd->sjkd", probs_low, grad_context, preferred_element_type=F32
    ).astype(BF16)
    inner_sum = jnp.sum(grad_probs * probs, axis=-1, keepdims=True)
    grad_scores = (probs * (grad_probs - inner_sum)).astype(BF16)
    grad_query = (
        jnp.einsum("skgij,sjkd->sikgd", grad_scores, key, preferred_element_type=F32)
        * softmax_scale
    ).reshape(groups, SLOT_LENGTH, heads, HEAD_SIZE)
    grad_key = (
        jnp.einsum("skgij,sikgd->sjkd", grad_scores, query, preferred_element_type=F32)
        * softmax_scale
    )
    grad_query_normed = grad_query * cosine + rotate_back(grad_query * sine)
    grad_key_normed = grad_key * cosine + rotate_back(grad_key * sine)
    grad_query_raw, query_gain_term = norm_back(
        grad_query_normed, query_unit, query_scale, gain_query
    )
    grad_key_raw, key_gain_term = norm_back(grad_key_normed, key_unit, key_scale, gain_key)
    rows = groups * SLOT_LENGTH
    grad_qkv = to_packed(
        jnp.concatenate(
            [
                grad_query_raw.astype(BF16).reshape(rows, q_cols),
                grad_key_raw.astype(BF16).reshape(rows, kv_cols),
                grad_value.reshape(rows, kv_cols),
            ],
            axis=1,
        )
    )
    qkv_term = dot_at(attention_input, grad_qkv).astype(BF16)
    grad_attn_in = scatter_sum(dot_bt(grad_qkv, w_qkv))
    grad_norm_one, gain_one_grad = norm_back(grad_attn_in, normed_one, scale_one, gain_one)
    input_grad = (grad_hidden + grad_norm_one).astype(BF16)

    def over_replicas(term):
        part = lax.psum_scatter(term, "rep", scatter_dimension=0, tiled=True)
        return lax.all_gather(part, "rep", axis=0, tiled=True).astype(F32)

    def columns_back(term):
        cols = term.shape[1]
        part = lax.psum_scatter(
            term.reshape(groups, shard, cols), "rep", scatter_dimension=1, tiled=True
        )
        part = lax.all_to_all(part, "fsdp", split_axis=0, concat_axis=0, tiled=True)
        full = lax.all_gather(part, "rep", axis=1, tiled=True)
        return jnp.swapaxes(full.astype(F32), 0, 1)

    down_share = over_replicas(down_term)
    ff_share = columns_back(ff_term)
    out_share = over_replicas(out_term)
    qkv_share = columns_back(qkv_term)

    def kv_share(part):
        part = part.reshape(shard, groups // spread, spread, kv_cols)
        return jnp.sum(part, axis=2).reshape(shard, KEY_VALUE_HEADS * HEAD_SIZE)

    gain_sums = lax.psum(
        jnp.concatenate([gain_one_grad, gain_two_grad, query_gain_term, key_gain_term]),
        ("rep", "fsdp"),
    )

    def own(start, length):
        return lax.dynamic_slice(gain_sums, (start + device * length,), (length,))

    return (
        output,
        input_grad,
        own(0, shard),
        qkv_share[:, :, :q_cols].reshape(shard, groups * q_cols),
        kv_share(qkv_share[:, :, q_cols : q_cols + kv_cols]),
        kv_share(qkv_share[:, :, q_cols + kv_cols :]),
        own(2 * width, head_part),
        own(2 * width + HEAD_SIZE, head_part),
        out_share,
        own(width, shard),
        ff_share[:, :, :ff_cols].reshape(shard, groups * ff_cols),
        ff_share[:, :, ff_cols:].reshape(shard, groups * ff_cols),
        down_share,
    )


def solution(mesh):
    rows = P(("rep", "fsdp"), None)
    vec = P("fsdp")
    mat = P("fsdp", None)
    return jax.shard_map(
        on_device,
        mesh=mesh,
        in_specs=(
            rows,
            rows,
            P("rep", None, None),
            P("rep", None),
            P("rep", "fsdp"),
            vec,
            mat,
            mat,
            mat,
            vec,
            vec,
            mat,
            vec,
            mat,
            mat,
            mat,
        ),
        out_specs=(rows, rows, vec, mat, mat, mat, vec, vec, mat, vec, mat, mat, mat),
        check_vma=False,
    )
```

```python
import functools

import jax
import jax.numpy as jnp
from jax import lax
from jax.experimental import pallas as pl
from jax.experimental.pallas import tpu as pltpu
from jax.sharding import PartitionSpec as P


QUERY_HEADS = 16
KEY_VALUE_HEADS = 8
HEAD_SIZE = 128
SLOT_LENGTH = 288

EPSILON = 1e-06
ROPE_BASE = 1000000.0
NEG_LARGE = -1e30

F32 = jnp.float32
BF16 = jnp.bfloat16


def rms_scale(values):
    return lax.rsqrt(jnp.mean(values * values, axis=-1, keepdims=True) + EPSILON)


def dot(left, right):
    return jnp.dot(left, right, preferred_element_type=F32)


def dot_bt(left, right):
    return lax.dot_general(left, right, (((1,), (1,)), ((), ())), preferred_element_type=F32)


def dot_at(left, right):
    return lax.dot_general(left, right, (((0,), (0,)), ((), ())), preferred_element_type=F32)


def norm_back(grad_normed, unit_rows, scale_rows, gain_rows):
    scaled = grad_normed * gain_rows
    return scale_rows * (
        scaled - unit_rows * jnp.mean(scaled * unit_rows, axis=-1, keepdims=True)
    )


def partners(me):
    core, x_bit, y_bit = lax.rem(me, 2), lax.rem(me // 2, 2), me // 4
    along_x = me + 2 - 4 * x_bit
    along_y = me + 4 - 8 * y_bit
    return me + 1 - 2 * core, along_x, along_y, along_x + 4 - 8 * y_bit


def greet(devices):
    barrier = pltpu.get_barrier_semaphore()
    for device in devices:
        pl.semaphore_signal(
            barrier, inc=1, device_id={"fsdp": device}, device_id_type=pl.DeviceIdType.MESH
        )
    pl.semaphore_wait(barrier, len(devices))


def gather_kernel(own, out, send, recv, local):
    me = lax.axis_index("fsdp")
    sib, along_x, along_y, across = partners(me)
    half = own.shape[1] // 2
    left, right = pl.ds(0, half), pl.ds(half, half)
    greet((sib, along_x, along_y))

    def copy(src, dst, slot, device):
        made = pltpu.make_async_remote_copy(
            src_ref=src,
            dst_ref=dst,
            send_sem=send.at[slot],
            recv_sem=recv.at[slot],
            device_id={"fsdp": device},
            device_id_type=pl.DeviceIdType.MESH,
        )
        made.start()
        return made

    mine = pltpu.make_async_copy(own, out.at[me], local)
    copies = [
        copy(own.at[:, left], out.at[me, :, left], 0, along_x),
        copy(own.at[:, right], out.at[me, :, right], 1, along_y),
        copy(own.at[:, right], out.at[me, :, right], 2, along_x),
        copy(own.at[:, left], out.at[me, :, left], 3, along_y),
        copy(own, out.at[me], 4, sib),
    ]
    mine.start()
    copies[0].wait_recv()
    copies.append(copy(out.at[along_x, :, left], out.at[along_x, :, left], 5, along_y))
    copies[1].wait_recv()
    copies.append(copy(out.at[along_y, :, right], out.at[along_y, :, right], 6, along_x))
    copies[2].wait_recv()
    copies.append(copy(out.at[along_x], out.at[along_x], 7, sib))
    copies[3].wait_recv()
    copies.append(copy(out.at[along_y], out.at[along_y], 8, sib))
    copies[5].wait_recv()
    copies[6].wait_recv()
    copies.append(copy(out.at[across], out.at[across], 9, sib))
    for slot in (4, 7, 8, 9):
        copies[slot].wait_recv()
    mine.wait()
    for made in copies:
        made.wait_send()


def gather_rows(values, ident):
    rows, cols = values.shape
    return pl.pallas_call(
        gather_kernel,
        out_shape=jax.ShapeDtypeStruct((8, rows, cols), values.dtype),
        in_specs=[pl.BlockSpec(memory_space=pltpu.VMEM)],
        out_specs=pl.BlockSpec(memory_space=pl.ANY),
        scratch_shapes=[
            pltpu.SemaphoreType.DMA((10,)),
            pltpu.SemaphoreType.DMA((10,)),
            pltpu.SemaphoreType.DMA,
        ],
        compiler_params=pltpu.CompilerParams(collective_id=ident, has_side_effects=True),
        cost_estimate=pl.CostEstimate(
            flops=0, bytes_accessed=rows * cols * 180, transcendentals=0
        ),
        name="gather_rows",
    )(values).reshape(8 * rows, cols)


def scatter_kernel(parts, out, mine, other, first, second, send, recv, local):
    me = lax.axis_index("fsdp")
    sib, along_x, along_y, across = partners(me)
    rows, cols = out.shape
    half = cols // 2
    left, right = pl.ds(0, half), pl.ds(half, half)
    order = (across, along_x, along_y, me)
    loads = []
    for step, device in enumerate(order):
        load = pltpu.make_async_copy(parts.at[device], mine.at[step], local.at[step])
        load.start()
        loads.append(load)
    greet((sib, along_x, along_y))

    def copy(src, dst, slot, device):
        made = pltpu.make_async_remote_copy(
            src_ref=src,
            dst_ref=dst,
            send_sem=send.at[slot],
            recv_sem=recv.at[slot],
            device_id={"fsdp": device},
            device_id_type=pl.DeviceIdType.MESH,
        )
        made.start()
        return made

    copies = [
        copy(parts.at[device + sib - me], other.at[step], step, sib)
        for step, device in enumerate(order)
    ]

    def add(into, term, step_rows=16):
        @pl.loop(0, rows // step_rows)
        def _(index):
            at = pl.ds(pl.multiple_of(index * step_rows, step_rows), step_rows)
            into[at, :] = (into[at, :].astype(F32) + term[at, :].astype(F32)).astype(into.dtype)

    def own_chip(step):
        loads[step].wait()
        copies[step].wait_recv()
        add(mine.at[step], other.at[step])

    own_chip(0)
    copies.append(copy(mine.at[0, :, left], first.at[0], 4, along_x))
    copies.append(copy(mine.at[0, :, right], first.at[1], 5, along_y))
    own_chip(1)
    copies.append(copy(mine.at[1, :, left], first.at[2], 6, along_x))
    own_chip(2)
    copies.append(copy(mine.at[2, :, right], first.at[3], 7, along_y))
    own_chip(3)
    copies[4].wait_recv()
    add(mine.at[2, :, left], first.at[0])
    copies.append(copy(mine.at[2, :, left], second.at[0], 8, along_y))
    copies[5].wait_recv()
    add(mine.at[1, :, right], first.at[1])
    copies.append(copy(mine.at[1, :, right], second.at[1], 9, along_x))
    copies[6].wait_recv()
    copies[7].wait_recv()
    copies[8].wait_recv()
    copies[9].wait_recv()

    @pl.loop(0, rows // 16)
    def _(index):
        at = pl.ds(pl.multiple_of(index * 16, 16), 16)
        for side, cut in enumerate((left, right)):
            out[at, cut] = (
                mine[3, at, cut].astype(F32)
                + first[2 + side, at, :].astype(F32)
                + second[side, at, :].astype(F32)
            )

    for made in copies:
        made.wait_send()


def scatter_rows(values, ident):
    rows, cols = values.shape[0] // 8, values.shape[1]
    return pl.pallas_call(
        scatter_kernel,
        out_shape=jax.ShapeDtypeStruct((rows, cols), F32),
        in_specs=[pl.BlockSpec(memory_space=pl.ANY)],
        out_specs=pl.BlockSpec(memory_space=pltpu.VMEM),
        scratch_shapes=[
            pltpu.VMEM((4, rows, cols), BF16),
            pltpu.VMEM((4, rows, cols), BF16),
            pltpu.VMEM((4, rows, cols // 2), BF16),
            pltpu.VMEM((2, rows, cols // 2), BF16),
            pltpu.SemaphoreType.DMA((10,)),
            pltpu.SemaphoreType.DMA((10,)),
            pltpu.SemaphoreType.DMA((4,)),
        ],
        compiler_params=pltpu.CompilerParams(collective_id=ident, has_side_effects=True),
        cost_estimate=pl.CostEstimate(
            flops=0, bytes_accessed=rows * cols * 200, transcendentals=0
        ),
        name="scatter_rows",
    )(values.astype(BF16).reshape(8, rows, cols))


class Deal:
    def __init__(self, starts, places, counts, in_rows, cap):
        self.starts, self.places, self.counts = starts, places, counts
        self.in_rows = in_rows
        self.window = (cap + 14) // 8 * 8

    def sources(self, run):
        for source in range(self.starts.shape[0]):
            yield (
                source * self.in_rows + self.starts[source, run],
                self.places[source, run],
                self.counts[source, run],
            )

    def move(self, src, dst, src_at, dst_at, count):
        window = self.window
        src_base = jnp.minimum(src_at // 8 * 8, src.shape[0] - window)
        dst_base = jnp.minimum(dst_at // 8 * 8, dst.shape[0] - window)
        lead = dst_at - dst_base
        shift = lax.rem(lead - (src_at - src_base) + window, window)
        rows = src[pl.ds(pl.multiple_of(src_base, 8), window), :]
        rows = pltpu.roll(rows, shift, 0)
        into = pl.ds(pl.multiple_of(dst_base, 8), window)
        row = lax.broadcasted_iota(jnp.int32, rows.shape, 0)
        keep = (row >= lead) & (row < lead + count)
        dst[into, :] = jnp.where(keep, rows, dst[into, :])

    def load(self, packed, slot, run):
        for start, place, count in self.sources(run):
            self.move(packed, slot, start, place, count)

    def store(self, packed, slot, run):
        for start, place, count in self.sources(run):
            self.move(slot, packed, place, start, count)

    def length(self, run):
        total = 0
        for source in range(self.starts.shape[0]):
            total = total + self.counts[source, run]
        return total


KEY_SPAN = 384
BLOCKS = ((0, 128, 128), (128, 256, 256), (256, 288, KEY_SPAN))


def rotate(values, cosine, sine):
    return values * cosine + pltpu.roll(values, HEAD_SIZE // 2, 1) * sine


def unrotate(values, cosine, sine):
    return values * cosine + pltpu.roll(values * sine, HEAD_SIZE // 2, 1)


def block_probs(query, key, first, last, span, length):
    scores = dot_bt(query[first:last], key[:span]) * HEAD_SIZE ** (-0.5)
    row = first + lax.broadcasted_iota(jnp.int32, scores.shape, 0)
    column = lax.broadcasted_iota(jnp.int32, scores.shape, 1)
    scores = jnp.where((column <= row) & (column < length), scores, NEG_LARGE)
    exps = jnp.exp(scores - jnp.max(scores, axis=-1, keepdims=True))
    return exps / jnp.sum(exps, axis=-1, keepdims=True)


def attention_kernel(in_rows, cap, starts, places, counts, raw, gains, trig, out, slot, result, packed):
    deal = Deal(starts, places, counts, in_rows, cap)
    heads = out.shape[1] // HEAD_SIZE
    slot[...] = jnp.zeros_like(slot)
    length_rows = SLOT_LENGTH

    @pl.loop(0, starts.shape[0])
    def _(run):
        deal.load(raw, slot, run)
        length = deal.length(run)
        cosine, sine = trig[0], trig[1]
        key_at = heads * HEAD_SIZE
        key_raw = slot[:KEY_SPAN, key_at : key_at + HEAD_SIZE]
        key = rotate(key_raw * rms_scale(key_raw) * gains[1:2, :], cosine, sine).astype(BF16)
        value = slot[:KEY_SPAN, key_at + HEAD_SIZE :].astype(BF16)
        for head in range(heads):
            cut = slice(head * HEAD_SIZE, (head + 1) * HEAD_SIZE)
            query_raw = slot[:length_rows, cut]
            query = rotate(
                query_raw * rms_scale(query_raw) * gains[0:1, :],
                cosine[:length_rows],
                sine[:length_rows],
            ).astype(BF16)
            for first, last, span in BLOCKS:
                probs = block_probs(query, key, first, last, span, length)
                result[first:last, cut] = dot(probs.astype(BF16), value[:span])
        deal.store(packed, result, run)

    out[...] = packed[...].astype(BF16)


def attention_back_kernel(
    in_rows, cap, starts, places, counts, raw, grads, gains, trig, out, gain_out,
    slot, grad_slot, result, packed, key_sum, value_sum,
):
    deal = Deal(starts, places, counts, in_rows, cap)
    heads = grads.shape[1] // HEAD_SIZE
    slot[...] = jnp.zeros_like(slot)
    grad_slot[...] = jnp.zeros_like(grad_slot)
    gain_out[...] = jnp.zeros_like(gain_out)
    rows = SLOT_LENGTH

    def norm_and_store(grad, raw_rows, gain_row, cut, cosine, sine, gain_at):
        scale = rms_scale(raw_rows)
        unit = raw_rows * scale
        normed = unrotate(grad * HEAD_SIZE ** (-0.5), cosine, sine)
        gain_out[gain_at : gain_at + 1, :] += jnp.sum(normed * unit, axis=0, keepdims=True)
        result[:rows, cut] = norm_back(normed, unit, scale, gain_row)

    @pl.loop(0, starts.shape[0])
    def _(run):
        deal.load(raw, slot, run)
        deal.load(grads, grad_slot, run)
        length = deal.length(run)
        cosine, sine = trig[0], trig[1]
        key_at = heads * HEAD_SIZE
        key_raw = slot[:KEY_SPAN, key_at : key_at + HEAD_SIZE]
        key = rotate(key_raw * rms_scale(key_raw) * gains[1:2, :], cosine, sine).astype(BF16)
        value = slot[:KEY_SPAN, key_at + HEAD_SIZE :].astype(BF16)
        key_sum[...] = jnp.zeros_like(key_sum)
        value_sum[...] = jnp.zeros_like(value_sum)
        inside = lax.broadcasted_iota(jnp.int32, (rows, HEAD_SIZE), 0) < length
        for head in range(heads):
            cut = slice(head * HEAD_SIZE, (head + 1) * HEAD_SIZE)
            query_raw = slot[:rows, cut]
            query = rotate(
                query_raw * rms_scale(query_raw) * gains[0:1, :], cosine[:rows], sine[:rows]
            ).astype(BF16)
            grad_context = jnp.where(inside, grad_slot[:rows, cut], 0.0).astype(BF16)
            pieces = []
            for first, last, span in BLOCKS:
                probs = block_probs(query, key, first, last, span, length)
                grad_rows = grad_context[first:last]
                grad_probs = dot_bt(grad_rows, value[:span])
                value_sum[:span, :] += dot_at(probs.astype(BF16), grad_rows)
                inner = jnp.sum(grad_probs * probs, axis=-1, keepdims=True)
                grad_scores = (probs * (grad_probs - inner)).astype(BF16)
                pieces.append(dot(grad_scores, key[:span]))
                key_sum[:span, :] += dot_at(grad_scores, query[first:last])
            norm_and_store(
                jnp.concatenate(pieces), query_raw, gains[0:1, :], cut, cosine[:rows], sine[:rows], 0
            )
        norm_and_store(
            key_sum[:rows, :],
            key_raw[:rows],
            gains[1:2, :],
            slice(key_at, key_at + HEAD_SIZE),
            cosine[:rows],
            sine[:rows],
            1,
        )
        result[:rows, key_at + HEAD_SIZE :] = value_sum[:rows, :]
        deal.store(packed, result, run)

    out[...] = packed[...].astype(BF16)


def call_attention(kernel, tables, arrays, outs, scratch, in_rows, flops):
    cap = SLOT_LENGTH // tables[0].shape[0]
    vmem = pl.BlockSpec(memory_space=pltpu.VMEM)
    moved = sum(a.size * a.dtype.itemsize for a in arrays)
    return pl.pallas_call(
        functools.partial(kernel, in_rows, cap),
        out_shape=outs,
        in_specs=[pl.BlockSpec(memory_space=pltpu.SMEM)] * 3 + [vmem] * len(arrays),
        out_specs=jax.tree.map(lambda _: vmem, outs),
        scratch_shapes=[pltpu.VMEM(shape, F32) for shape in scratch],
        compiler_params=pltpu.CompilerParams(vmem_limit_bytes=48 << 20),
        cost_estimate=pl.CostEstimate(flops=flops, bytes_accessed=moved, transcendentals=1 << 20),
    )(*tables, *arrays)


def on_device(
    tokens,
    cotangent,
    counts,
    deal_order,
    seq_lengths,
    input_gain,
    w_query,
    key_projection,
    value_projection,
    query_gain,
    key_gain,
    w_out,
    mlp_gain,
    w_gate,
    w_up,
    w_down,
):
    groups = lax.axis_size("fsdp")
    replicas = lax.axis_size("rep")
    in_rows, width = tokens.shape
    shard = width // groups
    heads = QUERY_HEADS // groups
    kv_heads = max(1, KEY_VALUE_HEADS // groups)
    spread = max(1, groups // KEY_VALUE_HEADS)
    q_cols, kv_cols = heads * HEAD_SIZE, kv_heads * HEAD_SIZE
    ff_cols = w_gate.shape[1] // groups

    def gather(values):
        if groups == 8:
            return gather_rows(values, 0 if values.shape[0] == in_rows else 2)
        return lax.all_gather(values, "fsdp", axis=0, tiled=True)

    def scatter_sum(values):
        if groups == 8:
            return scatter_rows(values, 1)
        return lax.psum_scatter(
            values.astype(BF16), "fsdp", scatter_dimension=0, tiled=True
        ).astype(F32)

    def replica_scatter(term, axis):
        return lax.psum_scatter(term, "rep", scatter_dimension=axis, tiled=True)

    def replica_gather(part):
        return lax.all_gather(part, "rep", axis=0, tiled=False)

    def columns_home(part):
        part = lax.all_to_all(part, "fsdp", split_axis=0, concat_axis=0, tiled=True)
        return replica_gather(part)

    head_part = HEAD_SIZE // groups
    gain_row = jnp.concatenate([input_gain, mlp_gain, query_gain, key_gain])
    gain_row = jnp.pad(gain_row[None], ((0, 15), (0, width - gain_row.shape[0])))
    got = gather(jnp.concatenate([tokens, gain_row])).reshape(groups, in_rows + 16, width)

    def kv_columns(weight):
        return jnp.repeat(
            weight.reshape(shard, KEY_VALUE_HEADS // kv_heads, kv_cols), spread, axis=1
        )

    send_attn = jnp.concatenate(
        [
            w_query.reshape(shard, groups, q_cols),
            kv_columns(key_projection),
            kv_columns(value_projection),
        ],
        axis=2,
    )
    w_qkv = lax.all_to_all(send_attn, "fsdp", split_axis=1, concat_axis=0, tiled=True).reshape(
        width, q_cols + 2 * kv_cols
    )
    send_ff = jnp.concatenate(
        [w_gate.reshape(shard, groups, ff_cols), w_up.reshape(shard, groups, ff_cols)], axis=2
    )
    piece = shard // replicas
    got, send_ff, cotangent_late = lax.optimization_barrier((got, send_ff, cotangent))
    all_grads = lax.all_gather(cotangent_late, "fsdp", axis=0, tiled=True)
    send_ff = lax.dynamic_slice(
        send_ff, (lax.axis_index("rep") * piece, 0, 0), (piece, groups, 2 * ff_cols)
    )
    w_ff = lax.all_to_all(send_ff, "fsdp", split_axis=1, concat_axis=0, tiled=False)
    w_ff = lax.all_gather(w_ff, "rep", axis=1, tiled=True).reshape(width, 2 * ff_cols)
    all_tokens = got[:, :in_rows].reshape(groups * in_rows, width)
    gains = got[:, in_rows].astype(F32)
    gain_one = gains[:, :shard].reshape(width)
    gain_two = gains[:, shard : 2 * shard].reshape(width)
    gain_query = gains[:, 2 * shard : 2 * shard + head_part].reshape(HEAD_SIZE)
    gain_key = gains[:, 2 * shard + head_part : 2 * (shard + head_part)].reshape(HEAD_SIZE)

    table = counts[0]
    tables = (
        jnp.cumsum(table, axis=1) - table,
        jnp.cumsum(table, axis=0) - table,
        table,
    )

    resid = tokens.astype(F32)
    scale_one = rms_scale(resid)
    normed_one = resid * scale_one
    all_resid = all_tokens.astype(F32)
    attention_input = (all_resid * rms_scale(all_resid) * gain_one).astype(BF16)
    raw = dot(attention_input, w_qkv)
    inverse = ROPE_BASE ** (-jnp.arange(0, HEAD_SIZE, 2, dtype=F32) / HEAD_SIZE)
    angles = jnp.arange(KEY_SPAN, dtype=F32)[:, None] * inverse
    cosine, sine = jnp.cos(angles), jnp.sin(angles)
    trig = jnp.stack(
        [jnp.concatenate([cosine, cosine], 1), jnp.concatenate([-sine, sine], 1)]
    )
    head_gains = jnp.stack([gain_query, gain_key])
    all_rows = groups * in_rows
    slot_rows = SLOT_LENGTH + HEAD_SIZE
    qkv_cols = q_cols + 2 * kv_cols
    context = call_attention(
        attention_kernel,
        tables,
        (raw, head_gains, trig),
        jax.ShapeDtypeStruct((all_rows, q_cols), BF16),
        ((slot_rows, qkv_cols), (slot_rows, q_cols), (all_rows, q_cols)),
        in_rows,
        4 * groups * heads * SLOT_LENGTH * SLOT_LENGTH * HEAD_SIZE,
    )
    hidden_one = resid + scatter_sum(dot(context, w_out))

    scale_two = rms_scale(hidden_one)
    normed_two = hidden_one * scale_two
    mlp_in = gather((normed_two * gain_two).astype(BF16))
    gate_pre = dot(mlp_in, w_ff[:, :ff_cols])
    up_pre = dot(mlp_in, w_ff[:, ff_cols:])
    sigmoid_gate = jax.nn.sigmoid(gate_pre)
    activ = (gate_pre * sigmoid_gate * up_pre).astype(BF16)

    grad_activ = dot_bt(all_grads, w_down)
    grad_gate = (
        grad_activ * up_pre * sigmoid_gate * (1.0 + gate_pre * (1.0 - sigmoid_gate))
    ).astype(BF16)
    grad_up = (grad_activ * (gate_pre * sigmoid_gate)).astype(BF16)
    grad_ff = jnp.concatenate([grad_gate, grad_up], axis=1)
    down_term = dot_at(activ, all_grads).astype(BF16)
    grad_ff, down_term = lax.optimization_barrier((grad_ff, down_term))
    down_part = replica_scatter(down_term, 0)
    ff_term = dot_at(mlp_in, grad_ff).astype(BF16)
    grad_ff, ff_term = lax.optimization_barrier((grad_ff, ff_term))
    ff_part = replica_scatter(ff_term.reshape(groups, shard, 2 * ff_cols), 1)
    grad_mlp_in = scatter_sum(dot_bt(grad_ff, w_ff))
    grad_norm_two = norm_back(grad_mlp_in, normed_two, scale_two, gain_two)
    grad_hidden = cotangent.astype(F32) + grad_norm_two

    all_hidden = gather(grad_hidden.astype(BF16))
    out_term = dot_at(context, all_hidden).astype(BF16)
    all_hidden, out_term = lax.optimization_barrier((all_hidden, out_term))
    out_part = replica_scatter(out_term, 0)
    grad_qkv, head_terms = call_attention(
        attention_back_kernel,
        tables,
        (raw, dot_bt(all_hidden, w_out), head_gains, trig),
        (
            jax.ShapeDtypeStruct((all_rows, qkv_cols), BF16),
            jax.ShapeDtypeStruct((8, HEAD_SIZE), F32),
        ),
        (
            (slot_rows, qkv_cols),
            (slot_rows, q_cols),
            (slot_rows, qkv_cols),
            (all_rows, qkv_cols),
            (KEY_SPAN, HEAD_SIZE),
            (KEY_SPAN, HEAD_SIZE),
        ),
        in_rows,
        10 * groups * heads * SLOT_LENGTH * SLOT_LENGTH * HEAD_SIZE,
    )
    qkv_term = dot_at(attention_input, grad_qkv).astype(BF16)

    def gain_column(weight, term, gain):
        return jnp.sum(weight.astype(F32) * term.astype(F32), axis=1) / gain

    def head_column(term):
        return jnp.pad(
            term.reshape(groups, head_part), ((0, 0), (0, shard - head_part))
        ).reshape(width)

    gain_terms = jnp.stack(
        [
            gain_column(w_qkv, qkv_term, gain_one),
            gain_column(w_ff, ff_term, gain_two),
            head_column(head_terms[0]),
            head_column(head_terms[1]),
        ],
        axis=1,
    )
    gain_terms = jnp.pad(gain_terms, ((0, 0), (0, HEAD_SIZE - 4)))
    small_term = jnp.concatenate([qkv_term, gain_terms.astype(BF16)], axis=1)
    grad_qkv, small_term, ff_part = lax.optimization_barrier((grad_qkv, small_term, ff_part))
    small_cols = small_term.shape[1]
    small_part = replica_scatter(small_term.reshape(groups, shard, small_cols), 1)
    ff_full = columns_home(ff_part)
    grad_attn_in = scatter_sum(dot_bt(grad_qkv, w_qkv))
    grad_norm_one = norm_back(grad_attn_in, normed_one, scale_one, gain_one)
    input_grad = (grad_hidden + grad_norm_one).astype(BF16)
    activ, grad_attn_in = lax.optimization_barrier((activ, grad_attn_in))
    output = (hidden_one + scatter_sum(dot(activ, w_down))).astype(BF16)

    down_share = replica_gather(down_part).reshape(w_down.shape).astype(F32)
    out_share = replica_gather(out_part).reshape(w_out.shape).astype(F32)
    small_full = columns_home(small_part)

    def columns(full, start, length):
        part = full[:, :, :, start : start + length].astype(F32)
        return jnp.swapaxes(part, 1, 2).reshape(shard, groups, length)

    def kv_share(start):
        part = columns(small_full, start, kv_cols)
        part = part.reshape(shard, groups // spread, spread, kv_cols)
        return jnp.sum(part, axis=2).reshape(shard, KEY_VALUE_HEADS * HEAD_SIZE)

    gain_sums = jnp.sum(small_full[:, :, :, qkv_cols:].astype(F32), axis=1)
    gain_sums = gain_sums.reshape(shard, HEAD_SIZE)
    ff_full = [columns(ff_full, start, ff_cols).reshape(shard, -1) for start in (0, ff_cols)]

    return (
        output,
        input_grad,
        gain_sums[:, 0],
        columns(small_full, 0, q_cols).reshape(shard, groups * q_cols),
        kv_share(q_cols),
        kv_share(q_cols + kv_cols),
        gain_sums[:head_part, 2],
        gain_sums[:head_part, 3],
        out_share,
        gain_sums[:, 1],
        ff_full[0],
        ff_full[1],
        down_share,
    )


def solution(mesh):
    rows = P(("rep", "fsdp"), None)
    vec = P("fsdp")
    mat = P("fsdp", None)
    return jax.shard_map(
        on_device,
        mesh=mesh,
        in_specs=(
            rows,
            rows,
            P("rep", None, None),
            P("rep", None),
            P("rep", "fsdp"),
            vec,
            mat,
            mat,
            mat,
            vec,
            vec,
            mat,
            vec,
            mat,
            mat,
            mat,
        ),
        out_specs=(rows, rows, vec, mat, mat, mat, vec, vec, mat, vec, mat, mat, mat),
        check_vma=False,
    )
```

```python
import functools

import jax
import jax.numpy as jnp
from jax import lax
from jax.experimental import pallas as pl
from jax.experimental.pallas import tpu as pltpu
from jax.sharding import PartitionSpec as P


QUERY_HEADS = 16
KEY_VALUE_HEADS = 8
HEAD_SIZE = 128
SLOT_LENGTH = 288

EPSILON = 1e-06
ROPE_BASE = 1000000.0
NEG_LARGE = -1e30

F32 = jnp.float32
BF16 = jnp.bfloat16


def rms_scale(values):
    return lax.rsqrt(jnp.mean(values * values, axis=-1, keepdims=True) + EPSILON)


def dot(left, right):
    return jnp.dot(left, right, preferred_element_type=F32)


def dot_bt(left, right):
    return lax.dot_general(left, right, (((1,), (1,)), ((), ())), preferred_element_type=F32)


def dot_at(left, right):
    return lax.dot_general(left, right, (((0,), (0,)), ((), ())), preferred_element_type=F32)


def norm_back(grad_normed, unit_rows, scale_rows, gain_rows):
    scaled = grad_normed * gain_rows
    return scale_rows * (
        scaled - unit_rows * jnp.mean(scaled * unit_rows, axis=-1, keepdims=True)
    )


def partners(me):
    core, x_bit, y_bit = lax.rem(me, 2), lax.rem(me // 2, 2), me // 4
    along_x = me + 2 - 4 * x_bit
    along_y = me + 4 - 8 * y_bit
    return me + 1 - 2 * core, along_x, along_y, along_x + 4 - 8 * y_bit


def greet(devices):
    barrier = pltpu.get_barrier_semaphore()
    for device in devices:
        pl.semaphore_signal(
            barrier, inc=1, device_id={"fsdp": device}, device_id_type=pl.DeviceIdType.MESH
        )
    pl.semaphore_wait(barrier, len(devices))


def send(src, dst, send_sem, recv_sem, device):
    made = pltpu.make_async_remote_copy(
        src_ref=src,
        dst_ref=dst,
        send_sem=send_sem,
        recv_sem=recv_sem,
        device_id={"fsdp": device},
        device_id_type=pl.DeviceIdType.MESH,
    )
    made.start()
    return made


def exchange_rows(own, out, sends, recvs, local, between=None):
    me = lax.axis_index("fsdp")
    sib, along_x, along_y, across = partners(me)
    half = own.shape[1] // 2
    left, right = pl.ds(0, half), pl.ds(half, half)

    def copy(src, dst, slot, device):
        return send(src, dst, sends.at[slot], recvs.at[slot], device)

    mine = pltpu.make_async_copy(own, out.at[me], local)
    copies = [
        copy(own.at[:, left], out.at[me, :, left], 0, along_x),
        copy(own.at[:, right], out.at[me, :, right], 1, along_y),
        copy(own.at[:, right], out.at[me, :, right], 2, along_x),
        copy(own.at[:, left], out.at[me, :, left], 3, along_y),
        copy(own, out.at[me], 4, sib),
    ]
    mine.start()
    copies[0].wait_recv()
    copies.append(copy(out.at[along_x, :, left], out.at[along_x, :, left], 5, along_y))
    copies[1].wait_recv()
    copies.append(copy(out.at[along_y, :, right], out.at[along_y, :, right], 6, along_x))
    if between:
        between()
    copies[2].wait_recv()
    copies.append(copy(out.at[along_x], out.at[along_x], 7, sib))
    copies[3].wait_recv()
    copies.append(copy(out.at[along_y], out.at[along_y], 8, sib))
    copies[5].wait_recv()
    copies[6].wait_recv()
    copies.append(copy(out.at[across], out.at[across], 9, sib))
    for slot in (4, 7, 8, 9):
        copies[slot].wait_recv()
    mine.wait()
    for made in copies:
        made.wait_send()


def gather_kernel(own, out, sends, recvs, local):
    greet(partners(lax.axis_index("fsdp"))[:3])
    exchange_rows(own, out, sends, recvs, local)


def gather_rows(values, ident):
    rows, cols = values.shape
    return pl.pallas_call(
        gather_kernel,
        out_shape=jax.ShapeDtypeStruct((8, rows, cols), values.dtype),
        in_specs=[pl.BlockSpec(memory_space=pltpu.VMEM)],
        out_specs=pl.BlockSpec(memory_space=pl.ANY),
        scratch_shapes=[
            pltpu.SemaphoreType.DMA((10,)),
            pltpu.SemaphoreType.DMA((10,)),
            pltpu.SemaphoreType.DMA,
        ],
        compiler_params=pltpu.CompilerParams(collective_id=ident, has_side_effects=True),
        cost_estimate=pl.CostEstimate(
            flops=0, bytes_accessed=rows * cols * 180, transcendentals=0
        ),
        name="gather_rows",
    )(values).reshape(8 * rows, cols)


def start_kernel(
    own, w_query, w_key, w_value, w_gate, w_up, out, w_qkv, w_ff,
    own_qkv, own_ff, sends, recvs, local, w_sends, w_recvs, w_local,
):
    me = lax.axis_index("fsdp")
    core, x_bit, y_bit = lax.rem(me, 2), lax.rem(me // 2, 2), me // 4
    shard = w_query.shape[0]
    piece = w_ff.shape[1]
    rows = pl.ds(pl.multiple_of(me * shard, shard), shard)
    part = pl.ds(pl.multiple_of(lax.axis_index("rep") * piece, piece), piece)
    pairs = []
    at = 0
    for weight in (w_query, w_key, w_value):
        cols = weight.shape[1] // 8
        pairs.append((weight, slice(None), cols, w_qkv.at[rows, at : at + cols], own_qkv, at))
        at += cols
    at = 0
    for weight in (w_gate, w_up):
        cols = weight.shape[1] // 8
        pairs.append((weight, part, cols, w_ff.at[me, :, at : at + cols], own_ff, at))
        at += cols

    def source(pair, device):
        weight, taken, cols = pair[:3]
        return weight.at[taken, pl.ds(pl.multiple_of(device * cols, cols), cols)]

    peers = []
    for flip in (6, 2, 4, 7, 3, 5, 1):
        bits = [
            1 - bit if flip >> place & 1 else bit
            for place, bit in enumerate((core, x_bit, y_bit))
        ]
        peers.append((flip - 1, bits[0] + 2 * bits[1] + 4 * bits[2]))
    into = [
        pltpu.make_async_copy(
            source(pair, me), pair[4].at[:, pair[5] : pair[5] + pair[2]], w_local.at[index]
        )
        for index, pair in enumerate(pairs)
    ]
    for made in into:
        made.start()
    greet([device for _, device in peers])
    copies = []

    def between():
        for chosen in ((0, 1, 2), (3, 4)):
            for slot, device in peers:
                for index in chosen:
                    copies.append(
                        send(
                            source(pairs[index], device),
                            pairs[index][3],
                            w_sends.at[slot, index],
                            w_recvs.at[slot, index],
                            device,
                        )
                    )

    exchange_rows(own, out, sends, recvs, local, between)
    for made in into:
        made.wait()
    home = [
        pltpu.make_async_copy(own_qkv, w_qkv.at[rows, :], w_local.at[0]),
        pltpu.make_async_copy(own_ff, w_ff.at[me], w_local.at[1]),
    ]
    for made in home:
        made.start()
    for made in copies:
        made.wait_recv()
    for made in copies:
        made.wait_send()
    for made in home:
        made.wait()


def start(values, weights, replicas, ident):
    rows, cols = values.shape
    shard = weights[0].shape[0]
    qkv_cols = sum(w.shape[1] for w in weights[:3]) // 8
    ff_cols = sum(w.shape[1] for w in weights[3:]) // 8
    anywhere = pl.BlockSpec(memory_space=pl.ANY)
    return pl.pallas_call(
        start_kernel,
        out_shape=(
            jax.ShapeDtypeStruct((8, rows, cols), values.dtype),
            jax.ShapeDtypeStruct((8 * shard, qkv_cols), BF16),
            jax.ShapeDtypeStruct((8, shard // replicas, ff_cols), BF16),
        ),
        in_specs=[pl.BlockSpec(memory_space=pltpu.VMEM)] + [anywhere] * 5,
        out_specs=(anywhere,) * 3,
        scratch_shapes=[
            pltpu.VMEM((shard, qkv_cols), BF16),
            pltpu.VMEM((shard // replicas, ff_cols), BF16),
            pltpu.SemaphoreType.DMA((10,)),
            pltpu.SemaphoreType.DMA((10,)),
            pltpu.SemaphoreType.DMA,
            pltpu.SemaphoreType.DMA((7, 5)),
            pltpu.SemaphoreType.DMA((7, 5)),
            pltpu.SemaphoreType.DMA((5,)),
        ],
        compiler_params=pltpu.CompilerParams(collective_id=ident, has_side_effects=True),
        cost_estimate=pl.CostEstimate(
            flops=0, bytes_accessed=rows * cols * 360, transcendentals=0
        ),
        name="start",
    )(values, *weights)


def scatter_kernel(parts, out, mine, other, first, second, send, recv, local):
    me = lax.axis_index("fsdp")
    sib, along_x, along_y, across = partners(me)
    rows, cols = out.shape
    half = cols // 2
    left, right = pl.ds(0, half), pl.ds(half, half)
    order = (across, along_x, along_y, me)
    loads = []
    for step, device in enumerate(order):
        load = pltpu.make_async_copy(parts.at[device], mine.at[step], local.at[step])
        load.start()
        loads.append(load)
    greet((sib, along_x, along_y))

    def copy(src, dst, slot, device):
        made = pltpu.make_async_remote_copy(
            src_ref=src,
            dst_ref=dst,
            send_sem=send.at[slot],
            recv_sem=recv.at[slot],
            device_id={"fsdp": device},
            device_id_type=pl.DeviceIdType.MESH,
        )
        made.start()
        return made

    copies = [
        copy(parts.at[device + sib - me], other.at[step], step, sib)
        for step, device in enumerate(order)
    ]

    def add(into, term, step_rows=16):
        @pl.loop(0, rows // step_rows)
        def _(index):
            at = pl.ds(pl.multiple_of(index * step_rows, step_rows), step_rows)
            into[at, :] = (into[at, :].astype(F32) + term[at, :].astype(F32)).astype(into.dtype)

    def own_chip(step):
        loads[step].wait()
        copies[step].wait_recv()
        add(mine.at[step], other.at[step])

    own_chip(0)
    copies.append(copy(mine.at[0, :, left], first.at[0], 4, along_x))
    copies.append(copy(mine.at[0, :, right], first.at[1], 5, along_y))
    own_chip(1)
    copies.append(copy(mine.at[1, :, left], first.at[2], 6, along_x))
    own_chip(2)
    copies.append(copy(mine.at[2, :, right], first.at[3], 7, along_y))
    own_chip(3)
    copies[4].wait_recv()
    add(mine.at[2, :, left], first.at[0])
    copies.append(copy(mine.at[2, :, left], second.at[0], 8, along_y))
    copies[5].wait_recv()
    add(mine.at[1, :, right], first.at[1])
    copies.append(copy(mine.at[1, :, right], second.at[1], 9, along_x))
    copies[6].wait_recv()
    copies[7].wait_recv()
    copies[8].wait_recv()
    copies[9].wait_recv()

    @pl.loop(0, rows // 16)
    def _(index):
        at = pl.ds(pl.multiple_of(index * 16, 16), 16)
        for side, cut in enumerate((left, right)):
            out[at, cut] = (
                mine[3, at, cut].astype(F32)
                + first[2 + side, at, :].astype(F32)
                + second[side, at, :].astype(F32)
            )

    for made in copies:
        made.wait_send()


def scatter_rows(values, ident):
    rows, cols = values.shape[0] // 8, values.shape[1]
    return pl.pallas_call(
        scatter_kernel,
        out_shape=jax.ShapeDtypeStruct((rows, cols), F32),
        in_specs=[pl.BlockSpec(memory_space=pl.ANY)],
        out_specs=pl.BlockSpec(memory_space=pltpu.VMEM),
        scratch_shapes=[
            pltpu.VMEM((4, rows, cols), BF16),
            pltpu.VMEM((4, rows, cols), BF16),
            pltpu.VMEM((4, rows, cols // 2), BF16),
            pltpu.VMEM((2, rows, cols // 2), BF16),
            pltpu.SemaphoreType.DMA((10,)),
            pltpu.SemaphoreType.DMA((10,)),
            pltpu.SemaphoreType.DMA((4,)),
        ],
        compiler_params=pltpu.CompilerParams(collective_id=ident, has_side_effects=True),
        cost_estimate=pl.CostEstimate(
            flops=0, bytes_accessed=rows * cols * 200, transcendentals=0
        ),
        name="scatter_rows",
    )(values.astype(BF16).reshape(8, rows, cols))


def place_kernel(widths, shared, got, *outs):
    at = 0
    for width, share, out in zip(widths, shared, outs):
        for place in range(got.shape[0] // share):
            total = got[place * share, :, at : at + width].astype(F32)
            for source in range(place * share + 1, (place + 1) * share):
                total = total + got[source, :, at : at + width].astype(F32)
            out[:, place * width : (place + 1) * width] = total
        at += width


def place_columns(full, widths, shared):
    replicas, groups, rows, cols = full.shape
    return pl.pallas_call(
        functools.partial(place_kernel, widths, shared),
        out_shape=[
            jax.ShapeDtypeStruct((replicas * rows, groups // share * width), F32)
            for width, share in zip(widths, shared)
        ],
        grid=(replicas,),
        in_specs=[pl.BlockSpec((None, groups, rows, cols), lambda i: (i, 0, 0, 0))],
        out_specs=[
            pl.BlockSpec((rows, groups // share * width), lambda i: (i, 0))
            for width, share in zip(widths, shared)
        ],
        cost_estimate=pl.CostEstimate(flops=0, bytes_accessed=full.size * 6, transcendentals=0),
        name="place_columns",
    )(full)


class Deal:
    def __init__(self, starts, places, counts, in_rows, cap):
        self.starts, self.places, self.counts = starts, places, counts
        self.in_rows = in_rows
        self.window = (cap + 14) // 8 * 8

    def sources(self, run):
        for source in range(self.starts.shape[0]):
            yield (
                source * self.in_rows + self.starts[source, run],
                self.places[source, run],
                self.counts[source, run],
            )

    def move(self, src, dst, src_at, dst_at, count):
        window = self.window
        src_base = jnp.minimum(src_at // 8 * 8, src.shape[0] - window)
        dst_base = jnp.minimum(dst_at // 8 * 8, dst.shape[0] - window)
        lead = dst_at - dst_base
        shift = lax.rem(lead - (src_at - src_base) + window, window)
        rows = src[pl.ds(pl.multiple_of(src_base, 8), window), :]
        rows = pltpu.roll(rows, shift, 0)
        into = pl.ds(pl.multiple_of(dst_base, 8), window)
        row = lax.broadcasted_iota(jnp.int32, rows.shape, 0)
        keep = (row >= lead) & (row < lead + count)
        dst[into, :] = jnp.where(keep, rows, dst[into, :])

    def load(self, packed, slot, run):
        for start, place, count in self.sources(run):
            self.move(packed, slot, start, place, count)

    def store(self, packed, slot, run):
        for start, place, count in self.sources(run):
            self.move(slot, packed, place, start, count)

    def length(self, run):
        total = 0
        for source in range(self.starts.shape[0]):
            total = total + self.counts[source, run]
        return total


KEY_SPAN = 384
BLOCKS = ((0, 128, 128), (128, 256, 256), (256, 288, KEY_SPAN))


def rotate(values, cosine, sine):
    return values * cosine + pltpu.roll(values, HEAD_SIZE // 2, 1) * sine


def unrotate(values, cosine, sine):
    return values * cosine + pltpu.roll(values * sine, HEAD_SIZE // 2, 1)


def block_probs(query, key, first, last, span, length):
    scores = dot_bt(query[first:last], key[:span]) * HEAD_SIZE ** (-0.5)
    row = first + lax.broadcasted_iota(jnp.int32, scores.shape, 0)
    column = lax.broadcasted_iota(jnp.int32, scores.shape, 1)
    scores = jnp.where((column <= row) & (column < length), scores, NEG_LARGE)
    exps = jnp.exp(scores - jnp.max(scores, axis=-1, keepdims=True))
    return exps / jnp.sum(exps, axis=-1, keepdims=True)


def attention_kernel(in_rows, cap, starts, places, counts, raw, gains, trig, out, slot, result, packed):
    deal = Deal(starts, places, counts, in_rows, cap)
    heads = out.shape[1] // HEAD_SIZE
    slot[...] = jnp.zeros_like(slot)
    length_rows = SLOT_LENGTH

    @pl.loop(0, starts.shape[0])
    def _(run):
        deal.load(raw, slot, run)
        length = deal.length(run)
        cosine, sine = trig[0], trig[1]
        key_at = heads * HEAD_SIZE
        key_raw = slot[:KEY_SPAN, key_at : key_at + HEAD_SIZE]
        key = rotate(key_raw * rms_scale(key_raw) * gains[1:2, :], cosine, sine).astype(BF16)
        value = slot[:KEY_SPAN, key_at + HEAD_SIZE :].astype(BF16)
        for head in range(heads):
            cut = slice(head * HEAD_SIZE, (head + 1) * HEAD_SIZE)
            query_raw = slot[:length_rows, cut]
            query = rotate(
                query_raw * rms_scale(query_raw) * gains[0:1, :],
                cosine[:length_rows],
                sine[:length_rows],
            ).astype(BF16)
            for first, last, span in BLOCKS:
                probs = block_probs(query, key, first, last, span, length)
                result[first:last, cut] = dot(probs.astype(BF16), value[:span])
        deal.store(packed, result, run)

    out[...] = packed[...].astype(BF16)


def attention_back_kernel(
    in_rows, cap, starts, places, counts, raw, grads, gains, trig, out, gain_out,
    slot, grad_slot, result, packed, key_sum, value_sum,
):
    deal = Deal(starts, places, counts, in_rows, cap)
    heads = grads.shape[1] // HEAD_SIZE
    slot[...] = jnp.zeros_like(slot)
    grad_slot[...] = jnp.zeros_like(grad_slot)
    gain_out[...] = jnp.zeros_like(gain_out)
    rows = SLOT_LENGTH

    def norm_and_store(grad, raw_rows, gain_row, cut, cosine, sine, gain_at):
        scale = rms_scale(raw_rows)
        unit = raw_rows * scale
        normed = unrotate(grad * HEAD_SIZE ** (-0.5), cosine, sine)
        gain_out[gain_at : gain_at + 1, :] += jnp.sum(normed * unit, axis=0, keepdims=True)
        result[:rows, cut] = norm_back(normed, unit, scale, gain_row)

    @pl.loop(0, starts.shape[0])
    def _(run):
        deal.load(raw, slot, run)
        deal.load(grads, grad_slot, run)
        length = deal.length(run)
        cosine, sine = trig[0], trig[1]
        key_at = heads * HEAD_SIZE
        key_raw = slot[:KEY_SPAN, key_at : key_at + HEAD_SIZE]
        key = rotate(key_raw * rms_scale(key_raw) * gains[1:2, :], cosine, sine).astype(BF16)
        value = slot[:KEY_SPAN, key_at + HEAD_SIZE :].astype(BF16)
        key_sum[...] = jnp.zeros_like(key_sum)
        value_sum[...] = jnp.zeros_like(value_sum)
        inside = lax.broadcasted_iota(jnp.int32, (rows, HEAD_SIZE), 0) < length
        for head in range(heads):
            cut = slice(head * HEAD_SIZE, (head + 1) * HEAD_SIZE)
            query_raw = slot[:rows, cut]
            query = rotate(
                query_raw * rms_scale(query_raw) * gains[0:1, :], cosine[:rows], sine[:rows]
            ).astype(BF16)
            grad_context = jnp.where(inside, grad_slot[:rows, cut], 0.0).astype(BF16)
            pieces = []
            for first, last, span in BLOCKS:
                probs = block_probs(query, key, first, last, span, length)
                grad_rows = grad_context[first:last]
                grad_probs = dot_bt(grad_rows, value[:span])
                value_sum[:span, :] += dot_at(probs.astype(BF16), grad_rows)
                inner = jnp.sum(grad_probs * probs, axis=-1, keepdims=True)
                grad_scores = (probs * (grad_probs - inner)).astype(BF16)
                pieces.append(dot(grad_scores, key[:span]))
                key_sum[:span, :] += dot_at(grad_scores, query[first:last])
            norm_and_store(
                jnp.concatenate(pieces), query_raw, gains[0:1, :], cut, cosine[:rows], sine[:rows], 0
            )
        norm_and_store(
            key_sum[:rows, :],
            key_raw[:rows],
            gains[1:2, :],
            slice(key_at, key_at + HEAD_SIZE),
            cosine[:rows],
            sine[:rows],
            1,
        )
        result[:rows, key_at + HEAD_SIZE :] = value_sum[:rows, :]
        deal.store(packed, result, run)

    out[...] = packed[...].astype(BF16)


def call_attention(kernel, tables, arrays, outs, scratch, in_rows, flops):
    cap = SLOT_LENGTH // tables[0].shape[0]
    vmem = pl.BlockSpec(memory_space=pltpu.VMEM)
    moved = sum(a.size * a.dtype.itemsize for a in arrays)
    return pl.pallas_call(
        functools.partial(kernel, in_rows, cap),
        out_shape=outs,
        in_specs=[pl.BlockSpec(memory_space=pltpu.SMEM)] * 3 + [vmem] * len(arrays),
        out_specs=jax.tree.map(lambda _: vmem, outs),
        scratch_shapes=[pltpu.VMEM(shape, F32) for shape in scratch],
        compiler_params=pltpu.CompilerParams(vmem_limit_bytes=48 << 20),
        cost_estimate=pl.CostEstimate(flops=flops, bytes_accessed=moved, transcendentals=1 << 20),
    )(*tables, *arrays)


def on_device(
    tokens,
    cotangent,
    counts,
    deal_order,
    seq_lengths,
    input_gain,
    w_query,
    key_projection,
    value_projection,
    query_gain,
    key_gain,
    w_out,
    mlp_gain,
    w_gate,
    w_up,
    w_down,
):
    groups = lax.axis_size("fsdp")
    replicas = lax.axis_size("rep")
    device = lax.axis_index("fsdp")
    in_rows, width = tokens.shape
    shard = width // groups
    heads = QUERY_HEADS // groups
    kv_heads = max(1, KEY_VALUE_HEADS // groups)
    spread = max(1, groups // KEY_VALUE_HEADS)
    q_cols, kv_cols = heads * HEAD_SIZE, kv_heads * HEAD_SIZE
    ff_cols = w_gate.shape[1] // groups

    def replica_gather(part):
        return lax.all_gather(part, "rep", axis=0, tiled=False)

    def gather(values):
        if groups != 8:
            return lax.all_gather(values, "fsdp", axis=0, tiled=True)
        return gather_rows(values, 0)

    def scatter_sum(values):
        if groups != 8:
            return lax.psum_scatter(
                values.astype(BF16), "fsdp", scatter_dimension=0, tiled=True
            ).astype(F32)
        return scatter_rows(values, 1)

    def replica_scatter(term, axis):
        return lax.psum_scatter(term, "rep", scatter_dimension=axis, tiled=True)

    def columns_home(part):
        part = lax.all_to_all(part, "fsdp", split_axis=0, concat_axis=0, tiled=True)
        return replica_gather(part)

    head_part = HEAD_SIZE // groups
    gain_row = jnp.concatenate([input_gain, mlp_gain, query_gain, key_gain])
    gain_row = jnp.pad(gain_row[None], ((0, 15), (0, width - gain_row.shape[0])))
    start_rows = jnp.concatenate([tokens, gain_row])
    if groups == 8:
        got, w_qkv, w_ff = start(
            start_rows,
            (w_query, key_projection, value_projection, w_gate, w_up),
            replicas,
            2,
        )
    else:
        got = gather(start_rows)
        kv_shape = (shard, KEY_VALUE_HEADS // kv_heads, kv_cols)
        keys = jnp.repeat(key_projection.reshape(kv_shape), spread, axis=1)
        values = jnp.repeat(value_projection.reshape(kv_shape), spread, axis=1)
        send_qkv = jnp.concatenate(
            [w_query.reshape(shard, groups, q_cols), keys, values], axis=2
        )
        w_qkv = lax.all_to_all(send_qkv, "fsdp", split_axis=1, concat_axis=0, tiled=True)
        w_qkv = w_qkv.reshape(width, q_cols + 2 * kv_cols)
        send_ff = jnp.concatenate(
            [w_gate.reshape(shard, groups, ff_cols), w_up.reshape(shard, groups, ff_cols)], axis=2
        )
        piece = shard // replicas
        send_ff = lax.dynamic_slice(
            send_ff, (lax.axis_index("rep") * piece, 0, 0), (piece, groups, 2 * ff_cols)
        )
        w_ff = lax.all_to_all(send_ff, "fsdp", split_axis=1, concat_axis=0, tiled=False)
        w_ff = w_ff.reshape(groups, piece, 2 * ff_cols)
    got = got.reshape(groups, in_rows + 16, width)
    got, cotangent_late = lax.optimization_barrier((got, cotangent))
    all_grads = lax.all_gather(cotangent_late, "fsdp", axis=0, tiled=True)
    w_ff = lax.all_gather(w_ff, "rep", axis=1, tiled=True).reshape(width, 2 * ff_cols)
    all_tokens = got[:, :in_rows].reshape(groups * in_rows, width)
    gains = got[:, in_rows].astype(F32)
    gain_one = gains[:, :shard].reshape(width)
    gain_two = gains[:, shard : 2 * shard].reshape(width)
    gain_query = gains[:, 2 * shard : 2 * shard + head_part].reshape(HEAD_SIZE)
    gain_key = gains[:, 2 * shard + head_part : 2 * (shard + head_part)].reshape(HEAD_SIZE)

    table = counts[0]
    tables = (
        jnp.cumsum(table, axis=1) - table,
        jnp.cumsum(table, axis=0) - table,
        table,
    )

    resid = tokens.astype(F32)
    scale_one = rms_scale(resid)
    normed_one = resid * scale_one
    all_resid = all_tokens.astype(F32)
    attention_input = (all_resid * rms_scale(all_resid) * gain_one).astype(BF16)
    raw = dot(attention_input, w_qkv)
    inverse = ROPE_BASE ** (-jnp.arange(0, HEAD_SIZE, 2, dtype=F32) / HEAD_SIZE)
    angles = jnp.arange(KEY_SPAN, dtype=F32)[:, None] * inverse
    cosine, sine = jnp.cos(angles), jnp.sin(angles)
    trig = jnp.stack(
        [jnp.concatenate([cosine, cosine], 1), jnp.concatenate([-sine, sine], 1)]
    )
    head_gains = jnp.stack([gain_query, gain_key])
    all_rows = groups * in_rows
    slot_rows = SLOT_LENGTH + HEAD_SIZE
    qkv_cols = q_cols + 2 * kv_cols
    context = call_attention(
        attention_kernel,
        tables,
        (raw, head_gains, trig),
        jax.ShapeDtypeStruct((all_rows, q_cols), BF16),
        ((slot_rows, qkv_cols), (slot_rows, q_cols), (all_rows, q_cols)),
        in_rows,
        4 * groups * heads * SLOT_LENGTH * SLOT_LENGTH * HEAD_SIZE,
    )
    hidden_one = resid + scatter_sum(dot(context, w_out))

    scale_two = rms_scale(hidden_one)
    normed_two = hidden_one * scale_two
    mlp_in = gather((normed_two * gain_two).astype(BF16))
    gate_pre = dot(mlp_in, w_ff[:, :ff_cols])
    up_pre = dot(mlp_in, w_ff[:, ff_cols:])
    sigmoid_gate = jax.nn.sigmoid(gate_pre)
    activ = (gate_pre * sigmoid_gate * up_pre).astype(BF16)

    grad_activ = dot_bt(all_grads, w_down)
    grad_gate = (
        grad_activ * up_pre * sigmoid_gate * (1.0 + gate_pre * (1.0 - sigmoid_gate))
    ).astype(BF16)
    grad_up = (grad_activ * (gate_pre * sigmoid_gate)).astype(BF16)
    grad_ff = jnp.concatenate([grad_gate, grad_up], axis=1)
    down_term = dot_at(activ, all_grads).astype(BF16)
    grad_ff, down_term = lax.optimization_barrier((grad_ff, down_term))
    down_part = replica_scatter(down_term, 0)
    ff_term = dot_at(mlp_in, grad_ff).astype(BF16)
    grad_ff, ff_term = lax.optimization_barrier((grad_ff, ff_term))
    ff_part = replica_scatter(ff_term.reshape(groups, shard, 2 * ff_cols), 1)
    grad_mlp_in = scatter_sum(dot_bt(grad_ff, w_ff))
    grad_norm_two = norm_back(grad_mlp_in, normed_two, scale_two, gain_two)
    grad_hidden = cotangent.astype(F32) + grad_norm_two

    all_hidden = gather(grad_hidden.astype(BF16))
    out_term = dot_at(context, all_hidden).astype(BF16)
    all_hidden, out_term = lax.optimization_barrier((all_hidden, out_term))
    out_part = replica_scatter(out_term, 0)
    grad_qkv, head_terms = call_attention(
        attention_back_kernel,
        tables,
        (raw, dot_bt(all_hidden, w_out), head_gains, trig),
        (
            jax.ShapeDtypeStruct((all_rows, qkv_cols), BF16),
            jax.ShapeDtypeStruct((8, HEAD_SIZE), F32),
        ),
        (
            (slot_rows, qkv_cols),
            (slot_rows, q_cols),
            (slot_rows, qkv_cols),
            (all_rows, qkv_cols),
            (KEY_SPAN, HEAD_SIZE),
            (KEY_SPAN, HEAD_SIZE),
        ),
        in_rows,
        10 * groups * heads * SLOT_LENGTH * SLOT_LENGTH * HEAD_SIZE,
    )
    qkv_term = dot_at(attention_input, grad_qkv).astype(BF16)

    def gain_column(weight, term, gain):
        return jnp.sum(weight.astype(F32) * term.astype(F32), axis=1) / gain

    small_term = qkv_term
    grad_qkv, small_term, ff_part = lax.optimization_barrier((grad_qkv, small_term, ff_part))
    small_cols = small_term.shape[1]
    small_part = replica_scatter(small_term.reshape(groups, shard, small_cols), 1)
    ff_full = columns_home(ff_part)
    grad_attn_in = scatter_sum(dot_bt(grad_qkv, w_qkv))
    grad_norm_one = norm_back(grad_attn_in, normed_one, scale_one, gain_one)
    input_grad = (grad_hidden + grad_norm_one).astype(BF16)
    activ, grad_attn_in = lax.optimization_barrier((activ, grad_attn_in))
    last_sum = scatter_sum(dot(activ, w_down))
    output = (hidden_one + last_sum).astype(BF16)
    small_part, last_sum = lax.optimization_barrier((small_part, last_sum))
    small_full = columns_home(small_part)
    down_full = replica_gather(down_part)
    out_full = replica_gather(out_part)

    gate_share, up_share = place_columns(ff_full, (ff_cols, ff_cols), (1, 1))
    query_share, key_share, value_share = place_columns(
        small_full, (q_cols, kv_cols, kv_cols), (1, spread, spread)
    )
    gain_terms = (
        gain_column(w_qkv, qkv_term, gain_one),
        gain_column(w_ff, ff_term, gain_two),
        head_terms[0],
        head_terms[1],
    )
    gain_terms, _ = lax.optimization_barrier((jnp.concatenate(gain_terms), last_sum))
    gain_sums = lax.psum(gain_terms, ("rep", "fsdp"))

    def own(first, length):
        return lax.dynamic_slice(gain_sums, (first + device * length,), (length,))

    return (
        output,
        input_grad,
        own(0, shard),
        query_share,
        key_share,
        value_share,
        own(2 * width, head_part),
        own(2 * width + HEAD_SIZE, head_part),
        out_full.reshape(w_out.shape).astype(F32),
        own(width, shard),
        gate_share,
        up_share,
        down_full.reshape(w_down.shape).astype(F32),
    )


def solution(mesh):
    rows = P(("rep", "fsdp"), None)
    vec = P("fsdp")
    mat = P("fsdp", None)
    return jax.shard_map(
        on_device,
        mesh=mesh,
        in_specs=(
            rows,
            rows,
            P("rep", None, None),
            P("rep", None),
            P("rep", "fsdp"),
            vec,
            mat,
            mat,
            mat,
            vec,
            vec,
            mat,
            vec,
            mat,
            mat,
            mat,
        ),
        out_specs=(rows, rows, vec, mat, mat, mat, vec, vec, mat, vec, mat, mat, mat),
        check_vma=False,
    )
```

```python
import functools
import math

import jax
import jax.numpy as jnp
from jax import lax
from jax.experimental import pallas as pl
from jax.experimental.pallas import tpu as pltpu
from jax.sharding import PartitionSpec as P


QUERY_HEADS = 16
KEY_VALUE_HEADS = 8
HEAD_SIZE = 128
SLOT_LENGTH = 288

EPSILON = 1e-06
ROPE_BASE = 1000000.0
NEG_LARGE = -1e30

F32 = jnp.float32
BF16 = jnp.bfloat16


def rms_scale(values):
    return lax.rsqrt(jnp.mean(values * values, axis=-1, keepdims=True) + EPSILON)


def dot(left, right):
    return jnp.dot(left, right, preferred_element_type=F32)


def dot_bt(left, right):
    return lax.dot_general(left, right, (((1,), (1,)), ((), ())), preferred_element_type=F32)


def dot_at(left, right):
    return lax.dot_general(left, right, (((0,), (0,)), ((), ())), preferred_element_type=F32)


def norm_back(grad_normed, unit_rows, scale_rows, gain_rows):
    scaled = grad_normed * gain_rows
    return scale_rows * (
        scaled - unit_rows * jnp.mean(scaled * unit_rows, axis=-1, keepdims=True)
    )


def partners(me):
    core, x_bit, y_bit = lax.rem(me, 2), lax.rem(me // 2, 2), me // 4
    along_x = me + 2 - 4 * x_bit
    along_y = me + 4 - 8 * y_bit
    return me + 1 - 2 * core, along_x, along_y, along_x + 4 - 8 * y_bit


def greet(devices):
    barrier = pltpu.get_barrier_semaphore()
    for device in devices:
        pl.semaphore_signal(
            barrier, inc=1, device_id={"fsdp": device}, device_id_type=pl.DeviceIdType.MESH
        )
    pl.semaphore_wait(barrier, len(devices))


def send(src, dst, send_sem, recv_sem, device):
    made = pltpu.make_async_remote_copy(
        src_ref=src,
        dst_ref=dst,
        send_sem=send_sem,
        recv_sem=recv_sem,
        device_id={"fsdp": device},
        device_id_type=pl.DeviceIdType.MESH,
    )
    made.start()
    return made


def exchange_rows(own, out, sends, recvs, local, between=None):
    me = lax.axis_index("fsdp")
    sib, along_x, along_y, across = partners(me)
    half = own.shape[1] // 2
    left, right = pl.ds(0, half), pl.ds(half, half)

    def copy(src, dst, slot, device):
        return send(src, dst, sends.at[slot], recvs.at[slot], device)

    mine = pltpu.make_async_copy(own, out.at[me], local)
    copies = [
        copy(own.at[:, left], out.at[me, :, left], 0, along_x),
        copy(own.at[:, right], out.at[me, :, right], 1, along_y),
        copy(own.at[:, right], out.at[me, :, right], 2, along_x),
        copy(own.at[:, left], out.at[me, :, left], 3, along_y),
        copy(own, out.at[me], 4, sib),
    ]
    mine.start()
    copies[0].wait_recv()
    copies.append(copy(out.at[along_x, :, left], out.at[along_x, :, left], 5, along_y))
    copies[1].wait_recv()
    copies.append(copy(out.at[along_y, :, right], out.at[along_y, :, right], 6, along_x))
    if between:
        between()
    copies[2].wait_recv()
    copies.append(copy(out.at[along_x], out.at[along_x], 7, sib))
    copies[3].wait_recv()
    copies.append(copy(out.at[along_y], out.at[along_y], 8, sib))
    copies[5].wait_recv()
    copies[6].wait_recv()
    copies.append(copy(out.at[across], out.at[across], 9, sib))
    for slot in (4, 7, 8, 9):
        copies[slot].wait_recv()
    mine.wait()
    for made in copies:
        made.wait_send()


def gather_kernel(own, out, sends, recvs, local):
    greet(partners(lax.axis_index("fsdp"))[:3])
    exchange_rows(own, out, sends, recvs, local)


def gather_rows(values, ident):
    rows, cols = values.shape
    return pl.pallas_call(
        gather_kernel,
        out_shape=jax.ShapeDtypeStruct((8, rows, cols), values.dtype),
        in_specs=[pl.BlockSpec(memory_space=pltpu.VMEM)],
        out_specs=pl.BlockSpec(memory_space=pl.ANY),
        scratch_shapes=[
            pltpu.SemaphoreType.DMA((10,)),
            pltpu.SemaphoreType.DMA((10,)),
            pltpu.SemaphoreType.DMA,
        ],
        compiler_params=pltpu.CompilerParams(collective_id=ident, has_side_effects=True),
        cost_estimate=pl.CostEstimate(
            flops=0, bytes_accessed=rows * cols * 180, transcendentals=0
        ),
        name="gather_rows",
    )(values).reshape(8 * rows, cols)


def flipped(me, flip):
    bits = (lax.rem(me, 2), lax.rem(me // 2, 2), me // 4)
    bits = [1 - bit if flip >> place & 1 else bit for place, bit in enumerate(bits)]
    return bits[0] + 2 * bits[1] + 4 * bits[2]


class Columns:
    def __init__(self, weights, taken, out, staged, sends, recvs, local):
        self.me = lax.axis_index("fsdp")
        self.weights, self.taken, self.out, self.staged = weights, taken, out, staged
        self.sends, self.recvs, self.local = sends, recvs, local
        self.peers = [(flip - 1, flipped(self.me, flip)) for flip in (6, 2, 4, 7, 3, 5, 1)]
        self.cuts = []
        at = 0
        for weight in weights:
            cols = weight.shape[1] // 8
            self.cuts.append(slice(at, at + cols))
            at += cols
        self.copies = []

    def source(self, index, device):
        cols = self.weights[index].shape[1] // 8
        return self.weights[index].at[
            self.taken, pl.ds(pl.multiple_of(device * cols, cols), cols)
        ]

    def stage(self):
        self.staging = [
            pltpu.make_async_copy(
                self.source(index, self.me), self.staged.at[:, cut], self.local.at[index]
            )
            for index, cut in enumerate(self.cuts)
        ]
        for made in self.staging:
            made.start()

    def send(self):
        for slot, device in self.peers:
            for index, cut in enumerate(self.cuts):
                self.copies.append(
                    send(
                        self.source(index, device),
                        self.out.at[self.me, :, cut],
                        self.sends.at[slot, index],
                        self.recvs.at[slot, index],
                        device,
                    )
                )

    def finish(self):
        for made in self.staging:
            made.wait()
        home = pltpu.make_async_copy(self.staged, self.out.at[self.me], self.local.at[0])
        home.start()
        for made in self.copies:
            made.wait_recv()
        for made in self.copies:
            made.wait_send()
        home.wait()


def columns_kernel(w_gate, w_up, *refs):
    piece = refs[0].shape[1]
    taken = pl.ds(pl.multiple_of(lax.axis_index("rep") * piece, piece), piece)
    parts = [
        Columns((weight,), taken, refs[index], *refs[2 + 4 * index : 6 + 4 * index])
        for index, weight in enumerate((w_gate, w_up))
    ]
    for columns in parts:
        columns.stage()
    greet([device for _, device in parts[0].peers])
    for columns in parts:
        columns.send()
    for columns in parts:
        columns.finish()


def start_kernel(
    own, w_query, w_key, w_value, out, w_qkv,
    staged, sends, recvs, local, w_sends, w_recvs, w_local,
):
    columns = Columns(
        (w_query, w_key, w_value), slice(None), w_qkv, staged, w_sends, w_recvs, w_local
    )
    columns.stage()
    greet([device for _, device in columns.peers])
    exchange_rows(own, out, sends, recvs, local, columns.send)
    columns.finish()


def columns_specs(weights, rows):
    cols = sum(w.shape[1] for w in weights) // 8
    count = len(weights)
    scratch = [
        pltpu.VMEM((rows, cols), BF16),
        pltpu.SemaphoreType.DMA((7, count)),
        pltpu.SemaphoreType.DMA((7, count)),
        pltpu.SemaphoreType.DMA((count,)),
    ]
    return jax.ShapeDtypeStruct((8, rows, cols), BF16), scratch


def send_columns(weights, rows, ident):
    specs = [columns_specs((weight,), rows) for weight in weights]
    anywhere = pl.BlockSpec(memory_space=pl.ANY)
    return pl.pallas_call(
        columns_kernel,
        out_shape=[shape for shape, _ in specs],
        in_specs=[anywhere] * len(weights),
        out_specs=[anywhere] * len(weights),
        scratch_shapes=sum([scratch for _, scratch in specs], []),
        compiler_params=pltpu.CompilerParams(collective_id=ident, has_side_effects=True),
        cost_estimate=pl.CostEstimate(
            flops=0, bytes_accessed=rows * weights[0].shape[1] * 120, transcendentals=0
        ),
        name="send_columns",
    )(*weights)


def width_of(shape):
    return shape.shape[-1]


def start(values, weights, ident):
    rows, cols = values.shape
    shape, scratch = columns_specs(weights, weights[0].shape[0])
    anywhere = pl.BlockSpec(memory_space=pl.ANY)
    got, w_qkv = pl.pallas_call(
        start_kernel,
        out_shape=(jax.ShapeDtypeStruct((8, rows, cols), values.dtype), shape),
        in_specs=[pl.BlockSpec(memory_space=pltpu.VMEM)] + [anywhere] * len(weights),
        out_specs=(anywhere,) * 2,
        scratch_shapes=[
            scratch[0],
            pltpu.SemaphoreType.DMA((10,)),
            pltpu.SemaphoreType.DMA((10,)),
            pltpu.SemaphoreType.DMA,
        ]
        + scratch[1:],
        compiler_params=pltpu.CompilerParams(collective_id=ident, has_side_effects=True),
        cost_estimate=pl.CostEstimate(
            flops=0, bytes_accessed=rows * cols * 300, transcendentals=0
        ),
        name="start",
    )(values, *weights)
    return got, w_qkv.reshape(-1, width_of(shape))


def scatter_kernel(parts, out, mine, other, first, second, send, recv, local):
    me = lax.axis_index("fsdp")
    sib, along_x, along_y, across = partners(me)
    rows, cols = out.shape
    half = cols // 2
    left, right = pl.ds(0, half), pl.ds(half, half)
    order = (across, along_x, along_y, me)
    loads = []
    for step, device in enumerate(order):
        load = pltpu.make_async_copy(parts.at[device], mine.at[step], local.at[step])
        load.start()
        loads.append(load)
    greet((sib, along_x, along_y))

    def copy(src, dst, slot, device):
        made = pltpu.make_async_remote_copy(
            src_ref=src,
            dst_ref=dst,
            send_sem=send.at[slot],
            recv_sem=recv.at[slot],
            device_id={"fsdp": device},
            device_id_type=pl.DeviceIdType.MESH,
        )
        made.start()
        return made

    copies = [
        copy(parts.at[device + sib - me], other.at[step], step, sib)
        for step, device in enumerate(order)
    ]

    def add(into, term, step_rows=16):
        @pl.loop(0, rows // step_rows)
        def _(index):
            at = pl.ds(pl.multiple_of(index * step_rows, step_rows), step_rows)
            into[at, :] = (into[at, :].astype(F32) + term[at, :].astype(F32)).astype(into.dtype)

    def own_chip(step):
        loads[step].wait()
        copies[step].wait_recv()
        add(mine.at[step], other.at[step])

    own_chip(0)
    copies.append(copy(mine.at[0, :, left], first.at[0], 4, along_x))
    copies.append(copy(mine.at[0, :, right], first.at[1], 5, along_y))
    own_chip(1)
    copies.append(copy(mine.at[1, :, left], first.at[2], 6, along_x))
    own_chip(2)
    copies.append(copy(mine.at[2, :, right], first.at[3], 7, along_y))
    own_chip(3)
    copies[4].wait_recv()
    add(mine.at[2, :, left], first.at[0])
    copies.append(copy(mine.at[2, :, left], second.at[0], 8, along_y))
    copies[5].wait_recv()
    add(mine.at[1, :, right], first.at[1])
    copies.append(copy(mine.at[1, :, right], second.at[1], 9, along_x))
    copies[6].wait_recv()
    copies[7].wait_recv()
    copies[8].wait_recv()
    copies[9].wait_recv()

    @pl.loop(0, rows // 16)
    def _(index):
        at = pl.ds(pl.multiple_of(index * 16, 16), 16)
        for side, cut in enumerate((left, right)):
            out[at, cut] = (
                mine[3, at, cut].astype(F32)
                + first[2 + side, at, :].astype(F32)
                + second[side, at, :].astype(F32)
            )

    for made in copies:
        made.wait_send()


def scatter_rows(values, ident):
    rows, cols = values.shape[0] // 8, values.shape[1]
    return pl.pallas_call(
        scatter_kernel,
        out_shape=jax.ShapeDtypeStruct((rows, cols), F32),
        in_specs=[pl.BlockSpec(memory_space=pl.ANY)],
        out_specs=pl.BlockSpec(memory_space=pltpu.VMEM),
        scratch_shapes=[
            pltpu.VMEM((4, rows, cols), BF16),
            pltpu.VMEM((4, rows, cols), BF16),
            pltpu.VMEM((4, rows, cols // 2), BF16),
            pltpu.VMEM((2, rows, cols // 2), BF16),
            pltpu.SemaphoreType.DMA((10,)),
            pltpu.SemaphoreType.DMA((10,)),
            pltpu.SemaphoreType.DMA((4,)),
        ],
        compiler_params=pltpu.CompilerParams(collective_id=ident, has_side_effects=True),
        cost_estimate=pl.CostEstimate(
            flops=0, bytes_accessed=rows * cols * 200, transcendentals=0
        ),
        name="scatter_rows",
    )(values.astype(BF16).reshape(8, rows, cols))


def place_kernel(widths, shared, got, *outs):
    at = 0
    for width, share, out in zip(widths, shared, outs):
        for place in range(got.shape[0] // share):
            total = got[place * share, :, at : at + width].astype(F32)
            for source in range(place * share + 1, (place + 1) * share):
                total = total + got[source, :, at : at + width].astype(F32)
            out[:, place * width : (place + 1) * width] = total
        at += width


def place_columns(full, widths, shared):
    replicas, groups, rows, cols = full.shape
    return pl.pallas_call(
        functools.partial(place_kernel, widths, shared),
        out_shape=[
            jax.ShapeDtypeStruct((replicas * rows, groups // share * width), F32)
            for width, share in zip(widths, shared)
        ],
        grid=(replicas,),
        in_specs=[pl.BlockSpec((None, groups, rows, cols), lambda i: (i, 0, 0, 0))],
        out_specs=[
            pl.BlockSpec((rows, groups // share * width), lambda i: (i, 0))
            for width, share in zip(widths, shared)
        ],
        cost_estimate=pl.CostEstimate(flops=0, bytes_accessed=full.size * 6, transcendentals=0),
        name="place_columns",
    )(full)


class Deal:
    def __init__(self, starts, places, counts, in_rows, cap):
        self.starts, self.places, self.counts = starts, places, counts
        self.in_rows = in_rows
        self.window = (cap + 14) // 8 * 8

    def sources(self, run):
        for source in range(self.starts.shape[0]):
            yield (
                source * self.in_rows + self.starts[source, run],
                self.places[source, run],
                self.counts[source, run],
            )

    def move(self, src, dst, src_at, dst_at, count):
        window = self.window
        src_base = jnp.minimum(src_at // 8 * 8, src.shape[0] - window)
        dst_base = jnp.minimum(dst_at // 8 * 8, dst.shape[0] - window)
        lead = dst_at - dst_base
        shift = lax.rem(lead - (src_at - src_base) + window, window)
        rows = src[pl.ds(pl.multiple_of(src_base, 8), window), :]
        rows = pltpu.roll(rows, shift, 0)
        into = pl.ds(pl.multiple_of(dst_base, 8), window)
        row = lax.broadcasted_iota(jnp.int32, rows.shape, 0)
        keep = (row >= lead) & (row < lead + count)
        dst[into, :] = jnp.where(keep, rows, dst[into, :])

    def load(self, packed, slot, run):
        for start, place, count in self.sources(run):
            self.move(packed, slot, start, place, count)

    def store(self, packed, slot, run):
        for start, place, count in self.sources(run):
            self.move(slot, packed, place, start, count)

    def length(self, run):
        total = 0
        for source in range(self.starts.shape[0]):
            total = total + self.counts[source, run]
        return total


KEY_SPAN = 384
BLOCKS = ((0, 128, 128), (128, 256, 256), (256, 288, KEY_SPAN))


def rotate(values, cosine, sine):
    return values * cosine + pltpu.roll(values, HEAD_SIZE // 2, 1) * sine


def unrotate(values, cosine, sine):
    return values * cosine + pltpu.roll(values * sine, HEAD_SIZE // 2, 1)


def block_probs(query, key, first, last, span, length):
    scores = dot_bt(query[first:last], key[:span]) * HEAD_SIZE ** (-0.5)
    row = first + lax.broadcasted_iota(jnp.int32, scores.shape, 0)
    column = lax.broadcasted_iota(jnp.int32, scores.shape, 1)
    scores = jnp.where((column <= row) & (column < length), scores, NEG_LARGE)
    exps = jnp.exp(scores - jnp.max(scores, axis=-1, keepdims=True))
    return exps / jnp.sum(exps, axis=-1, keepdims=True)


def attention_kernel(in_rows, cap, starts, places, counts, raw, gains, trig, out, slot, result, packed):
    deal = Deal(starts, places, counts, in_rows, cap)
    heads = out.shape[1] // HEAD_SIZE
    slot[...] = jnp.zeros_like(slot)
    length_rows = SLOT_LENGTH

    @pl.loop(0, starts.shape[0])
    def _(run):
        deal.load(raw, slot, run)
        length = deal.length(run)
        cosine, sine = trig[0], trig[1]
        key_at = heads * HEAD_SIZE
        key_raw = slot[:KEY_SPAN, key_at : key_at + HEAD_SIZE]
        key = rotate(key_raw * rms_scale(key_raw) * gains[1:2, :], cosine, sine).astype(BF16)
        value = slot[:KEY_SPAN, key_at + HEAD_SIZE :].astype(BF16)
        for head in range(heads):
            cut = slice(head * HEAD_SIZE, (head + 1) * HEAD_SIZE)
            query_raw = slot[:length_rows, cut]
            query = rotate(
                query_raw * rms_scale(query_raw) * gains[0:1, :],
                cosine[:length_rows],
                sine[:length_rows],
            ).astype(BF16)
            for first, last, span in BLOCKS:
                probs = block_probs(query, key, first, last, span, length)
                result[first:last, cut] = dot(probs.astype(BF16), value[:span])
        deal.store(packed, result, run)

    out[...] = packed[...].astype(BF16)


def attention_back_kernel(
    in_rows, cap, starts, places, counts, raw, grads, gains, trig, out, gain_out,
    slot, grad_slot, result, packed, key_sum, value_sum,
):
    deal = Deal(starts, places, counts, in_rows, cap)
    heads = grads.shape[1] // HEAD_SIZE
    slot[...] = jnp.zeros_like(slot)
    grad_slot[...] = jnp.zeros_like(grad_slot)
    gain_out[...] = jnp.zeros_like(gain_out)
    rows = SLOT_LENGTH

    def norm_and_store(grad, raw_rows, gain_row, cut, cosine, sine, gain_at):
        scale = rms_scale(raw_rows)
        unit = raw_rows * scale
        normed = unrotate(grad * HEAD_SIZE ** (-0.5), cosine, sine)
        gain_out[gain_at : gain_at + 1, :] += jnp.sum(normed * unit, axis=0, keepdims=True)
        result[:rows, cut] = norm_back(normed, unit, scale, gain_row)

    @pl.loop(0, starts.shape[0])
    def _(run):
        deal.load(raw, slot, run)
        deal.load(grads, grad_slot, run)
        length = deal.length(run)
        cosine, sine = trig[0], trig[1]
        key_at = heads * HEAD_SIZE
        key_raw = slot[:KEY_SPAN, key_at : key_at + HEAD_SIZE]
        key = rotate(key_raw * rms_scale(key_raw) * gains[1:2, :], cosine, sine).astype(BF16)
        value = slot[:KEY_SPAN, key_at + HEAD_SIZE :].astype(BF16)
        key_sum[...] = jnp.zeros_like(key_sum)
        value_sum[...] = jnp.zeros_like(value_sum)
        inside = lax.broadcasted_iota(jnp.int32, (rows, HEAD_SIZE), 0) < length
        for head in range(heads):
            cut = slice(head * HEAD_SIZE, (head + 1) * HEAD_SIZE)
            query_raw = slot[:rows, cut]
            query = rotate(
                query_raw * rms_scale(query_raw) * gains[0:1, :], cosine[:rows], sine[:rows]
            ).astype(BF16)
            grad_context = jnp.where(inside, grad_slot[:rows, cut], 0.0).astype(BF16)
            pieces = []
            for first, last, span in BLOCKS:
                probs = block_probs(query, key, first, last, span, length)
                grad_rows = grad_context[first:last]
                grad_probs = dot_bt(grad_rows, value[:span])
                value_sum[:span, :] += dot_at(probs.astype(BF16), grad_rows)
                inner = jnp.sum(grad_probs * probs, axis=-1, keepdims=True)
                grad_scores = (probs * (grad_probs - inner)).astype(BF16)
                pieces.append(dot(grad_scores, key[:span]))
                key_sum[:span, :] += dot_at(grad_scores, query[first:last])
            norm_and_store(
                jnp.concatenate(pieces), query_raw, gains[0:1, :], cut, cosine[:rows], sine[:rows], 0
            )
        norm_and_store(
            key_sum[:rows, :],
            key_raw[:rows],
            gains[1:2, :],
            slice(key_at, key_at + HEAD_SIZE),
            cosine[:rows],
            sine[:rows],
            1,
        )
        result[:rows, key_at + HEAD_SIZE :] = value_sum[:rows, :]
        deal.store(packed, result, run)

    out[...] = packed[...].astype(BF16)


def call_attention(kernel, tables, arrays, outs, scratch, in_rows, flops):
    cap = SLOT_LENGTH // tables[0].shape[0]
    vmem = pl.BlockSpec(memory_space=pltpu.VMEM)
    moved = sum(a.size * a.dtype.itemsize for a in arrays)
    return pl.pallas_call(
        functools.partial(kernel, in_rows, cap),
        out_shape=outs,
        in_specs=[pl.BlockSpec(memory_space=pltpu.SMEM)] * 3 + [vmem] * len(arrays),
        out_specs=jax.tree.map(lambda _: vmem, outs),
        scratch_shapes=[pltpu.VMEM(shape, F32) for shape in scratch],
        compiler_params=pltpu.CompilerParams(vmem_limit_bytes=48 << 20),
        cost_estimate=pl.CostEstimate(flops=flops, bytes_accessed=moved, transcendentals=1 << 20),
    )(*tables, *arrays)


def project_kernel(got, gain, weight, normed, raw):
    rows = got[: normed.shape[0], :].astype(F32)
    low = (rows * rms_scale(rows) * gain[...]).astype(BF16)
    normed[...] = low
    raw[...] = dot(low, weight[...])


def project(got, gain, weight, in_rows):
    groups, block, width = got.shape
    cols = weight.shape[1]
    return pl.pallas_call(
        project_kernel,
        out_shape=(
            jax.ShapeDtypeStruct((groups * in_rows, width), BF16),
            jax.ShapeDtypeStruct((groups * in_rows, cols), F32),
        ),
        grid=(groups,),
        in_specs=[
            pl.BlockSpec((None, block, width), lambda i: (i, 0, 0)),
            pl.BlockSpec((1, width), lambda i: (0, 0)),
            pl.BlockSpec((width, cols), lambda i: (0, 0)),
        ],
        out_specs=(
            pl.BlockSpec((in_rows, width), lambda i: (i, 0)),
            pl.BlockSpec((in_rows, cols), lambda i: (i, 0)),
        ),
        cost_estimate=pl.CostEstimate(
            flops=2 * groups * in_rows * width * cols,
            bytes_accessed=4 * got.size,
            transcendentals=0,
        ),
        name="project",
    )(got, gain[None], weight)


def feed_forward_kernel(rows, grads, w_gate, w_up, w_down, activ, grad_in):
    cols = activ.shape[1]
    step = cols // 3
    for at in range(0, cols, step):
        gate = dot(rows[...], w_gate[:, at : at + step])
        up = dot(rows[...], w_up[:, at : at + step])
        grad = dot_bt(grads[...], w_down[at : at + step, :])
        sigmoid = jax.nn.sigmoid(gate)
        silu = gate * sigmoid
        activ[:, at : at + step] = (silu * up).astype(BF16)
        grad_in[:, at : at + step] = (
            grad * up * sigmoid * (1.0 + gate * (1.0 - sigmoid))
        ).astype(BF16)
        grad_in[:, cols + at : cols + at + step] = (grad * silu).astype(BF16)


def feed_forward(rows, grads, w_gate, w_up, w_down, block):
    total, width = rows.shape
    cols = w_down.shape[0]
    row_spec = pl.BlockSpec((block, width), lambda i: (i, 0))
    return pl.pallas_call(
        feed_forward_kernel,
        out_shape=(
            jax.ShapeDtypeStruct((total, cols), BF16),
            jax.ShapeDtypeStruct((total, 2 * cols), BF16),
        ),
        grid=(total // block,),
        in_specs=[
            row_spec,
            row_spec,
            pl.BlockSpec(w_gate.shape, lambda i: (0, 0), pipeline_mode=pl.Buffered(1)),
            pl.BlockSpec(w_up.shape, lambda i: (0, 0), pipeline_mode=pl.Buffered(1)),
            pl.BlockSpec(w_down.shape, lambda i: (0, 0), pipeline_mode=pl.Buffered(1)),
        ],
        out_specs=(
            pl.BlockSpec((block, cols), lambda i: (i, 0)),
            pl.BlockSpec((block, 2 * cols), lambda i: (i, 0)),
        ),
        compiler_params=pltpu.CompilerParams(vmem_limit_bytes=48 << 20),
        cost_estimate=pl.CostEstimate(
            flops=6 * total * width * cols,
            bytes_accessed=4 * rows.size + 6 * w_down.size,
            transcendentals=total * cols,
        ),
        name="feed_forward",
    )(rows, grads, w_gate, w_up, w_down)


def input_grad_kernel(grads, w_gate, w_up, out):
    cols = w_gate.shape[1]
    gate, up = grads[:, :cols], grads[:, cols:]
    step = 512
    for at in range(0, out.shape[1], step):
        rows = slice(at, at + step)
        out[:, rows] = (dot_bt(gate, w_gate[rows, :]) + dot_bt(up, w_up[rows, :])).astype(BF16)


def input_grad_of(grads, w_gate, w_up, block):
    total, cols = grads.shape
    width = w_gate.shape[0]
    return pl.pallas_call(
        input_grad_kernel,
        out_shape=jax.ShapeDtypeStruct((total, width), BF16),
        grid=(total // block,),
        in_specs=[
            pl.BlockSpec((block, cols), lambda i: (i, 0)),
            pl.BlockSpec(w_gate.shape, lambda i: (0, 0), pipeline_mode=pl.Buffered(1)),
            pl.BlockSpec(w_up.shape, lambda i: (0, 0), pipeline_mode=pl.Buffered(1)),
        ],
        out_specs=pl.BlockSpec((block, width), lambda i: (i, 0)),
        compiler_params=pltpu.CompilerParams(vmem_limit_bytes=48 << 20),
        cost_estimate=pl.CostEstimate(
            flops=2 * total * width * cols,
            bytes_accessed=2 * grads.size + 2 * total * width + 4 * w_gate.size,
            transcendentals=0,
        ),
        name="input_grad",
    )(grads, w_gate, w_up)


def on_device(
    tokens,
    cotangent,
    counts,
    deal_order,
    seq_lengths,
    input_gain,
    w_query,
    key_projection,
    value_projection,
    query_gain,
    key_gain,
    w_out,
    mlp_gain,
    w_gate,
    w_up,
    w_down,
):
    groups = lax.axis_size("fsdp")
    replicas = lax.axis_size("rep")
    device = lax.axis_index("fsdp")
    in_rows, width = tokens.shape
    shard = width // groups
    heads = QUERY_HEADS // groups
    kv_heads = max(1, KEY_VALUE_HEADS // groups)
    spread = max(1, groups // KEY_VALUE_HEADS)
    q_cols, kv_cols = heads * HEAD_SIZE, kv_heads * HEAD_SIZE
    ff_cols = w_gate.shape[1] // groups

    def replica_gather(part):
        return lax.all_gather(part, "rep", axis=0, tiled=False)

    def gather(values):
        if groups != 8:
            return lax.all_gather(values, "fsdp", axis=0, tiled=True)
        return gather_rows(values, 0)

    def scatter_sum(values):
        if groups != 8:
            return lax.psum_scatter(
                values.astype(BF16), "fsdp", scatter_dimension=0, tiled=True
            ).astype(F32)
        return scatter_rows(values, 1)

    def replica_scatter(term, axis):
        return lax.psum_scatter(term, "rep", scatter_dimension=axis, tiled=True)

    def columns_home(part):
        part = lax.all_to_all(part, "fsdp", split_axis=0, concat_axis=0, tiled=True)
        return replica_gather(part)

    head_part = HEAD_SIZE // groups
    gain_row = jnp.concatenate([input_gain, mlp_gain, query_gain, key_gain])
    gain_row = jnp.pad(gain_row[None], ((0, 15), (0, width - gain_row.shape[0])))
    start_rows = jnp.concatenate([tokens, gain_row])
    if groups == 8:
        w_ff = send_columns((w_gate, w_up), shard // replicas, 3)
        start_rows, w_ff = lax.optimization_barrier((start_rows, w_ff))
        got, w_qkv = start(start_rows, (w_query, key_projection, value_projection), 2)
    else:
        got = gather(start_rows)
        kv_shape = (shard, KEY_VALUE_HEADS // kv_heads, kv_cols)
        keys = jnp.repeat(key_projection.reshape(kv_shape), spread, axis=1)
        values = jnp.repeat(value_projection.reshape(kv_shape), spread, axis=1)
        send_qkv = jnp.concatenate(
            [w_query.reshape(shard, groups, q_cols), keys, values], axis=2
        )
        w_qkv = lax.all_to_all(send_qkv, "fsdp", split_axis=1, concat_axis=0, tiled=True)
        w_qkv = w_qkv.reshape(width, q_cols + 2 * kv_cols)
        send_ff = jnp.concatenate(
            [w_gate.reshape(shard, groups, ff_cols), w_up.reshape(shard, groups, ff_cols)], axis=2
        )
        piece = shard // replicas
        send_ff = lax.dynamic_slice(
            send_ff, (lax.axis_index("rep") * piece, 0, 0), (piece, groups, 2 * ff_cols)
        )
        w_ff = lax.all_to_all(send_ff, "fsdp", split_axis=1, concat_axis=0, tiled=False)
        w_ff = w_ff.reshape(groups, piece, 2 * ff_cols)
        w_ff = (w_ff[:, :, :ff_cols], w_ff[:, :, ff_cols:])
    got = got.reshape(groups, in_rows + 16, width)
    got, cotangent_late = lax.optimization_barrier((got, cotangent))
    all_grads = lax.all_gather(cotangent_late, "fsdp", axis=0, tiled=True)

    def weight_columns(part):
        return lax.all_gather(part, "rep", axis=1, tiled=True).reshape(width, ff_cols)

    gate_cols = weight_columns(w_ff[0])
    up_cols = weight_columns(w_ff[1])
    gains = got[:, in_rows].astype(F32)
    gain_one = gains[:, :shard].reshape(width)
    gain_two = gains[:, shard : 2 * shard].reshape(width)
    gain_query = gains[:, 2 * shard : 2 * shard + head_part].reshape(HEAD_SIZE)
    gain_key = gains[:, 2 * shard + head_part : 2 * (shard + head_part)].reshape(HEAD_SIZE)

    table = counts[0]
    tables = (
        jnp.cumsum(table, axis=1) - table,
        jnp.cumsum(table, axis=0) - table,
        table,
    )

    resid = tokens.astype(F32)
    scale_one = rms_scale(resid)
    normed_one = resid * scale_one
    attention_input, raw = project(got, gain_one, w_qkv, in_rows)
    inverse = ROPE_BASE ** (-jnp.arange(0, HEAD_SIZE, 2, dtype=F32) / HEAD_SIZE)
    angles = jnp.arange(KEY_SPAN, dtype=F32)[:, None] * inverse
    cosine, sine = jnp.cos(angles), jnp.sin(angles)
    trig = jnp.stack(
        [jnp.concatenate([cosine, cosine], 1), jnp.concatenate([-sine, sine], 1)]
    )
    head_gains = jnp.stack([gain_query, gain_key])
    all_rows = groups * in_rows
    slot_rows = SLOT_LENGTH + HEAD_SIZE
    qkv_cols = q_cols + 2 * kv_cols
    context = call_attention(
        attention_kernel,
        tables,
        (raw, head_gains, trig),
        jax.ShapeDtypeStruct((all_rows, q_cols), BF16),
        ((slot_rows, qkv_cols), (slot_rows, q_cols), (all_rows, q_cols)),
        in_rows,
        4 * groups * heads * SLOT_LENGTH * SLOT_LENGTH * HEAD_SIZE,
    )
    hidden_one = resid + scatter_sum(dot(context, w_out))

    scale_two = rms_scale(hidden_one)
    normed_two = hidden_one * scale_two
    mlp_in = gather((normed_two * gain_two).astype(BF16))
    activ, grad_ff = feed_forward(mlp_in, all_grads, gate_cols, up_cols, w_down, in_rows)

    down_term = dot_at(activ, all_grads).astype(BF16)
    grad_ff, down_term = lax.optimization_barrier((grad_ff, down_term))
    down_part = replica_scatter(down_term, 0)
    ff_term = dot_at(mlp_in, grad_ff).astype(BF16)
    grad_ff, ff_term = lax.optimization_barrier((grad_ff, ff_term))
    ff_part = replica_scatter(ff_term.reshape(groups, shard, 2 * ff_cols), 1)
    grad_mlp_in = scatter_sum(input_grad_of(grad_ff, gate_cols, up_cols, in_rows))
    grad_norm_two = norm_back(grad_mlp_in, normed_two, scale_two, gain_two)
    grad_hidden = cotangent.astype(F32) + grad_norm_two

    all_hidden = gather(grad_hidden.astype(BF16))
    out_term = dot_at(context, all_hidden).astype(BF16)
    all_hidden, out_term = lax.optimization_barrier((all_hidden, out_term))
    grad_qkv, head_terms = call_attention(
        attention_back_kernel,
        tables,
        (raw, dot_bt(all_hidden, w_out), head_gains, trig),
        (
            jax.ShapeDtypeStruct((all_rows, qkv_cols), BF16),
            jax.ShapeDtypeStruct((8, HEAD_SIZE), F32),
        ),
        (
            (slot_rows, qkv_cols),
            (slot_rows, q_cols),
            (slot_rows, qkv_cols),
            (all_rows, qkv_cols),
            (KEY_SPAN, HEAD_SIZE),
            (KEY_SPAN, HEAD_SIZE),
        ),
        in_rows,
        10 * groups * heads * SLOT_LENGTH * SLOT_LENGTH * HEAD_SIZE,
    )
    qkv_term = dot_at(attention_input, grad_qkv).astype(BF16)

    def gain_column(weight, term, gain):
        return jnp.sum(weight.astype(F32) * term.astype(F32), axis=1) / gain

    small_term = qkv_term
    grad_qkv, small_term, ff_part = lax.optimization_barrier((grad_qkv, small_term, ff_part))
    piece = shard // replicas
    small_term = small_term.reshape(groups, replicas, piece, qkv_cols)
    lane = math.gcd(qkv_cols, width)
    small_term = jnp.swapaxes(small_term, 0, 1).reshape(replicas, -1, lane)
    small_rows = small_term.shape[1]
    rest_term = jnp.concatenate([small_term, out_term.reshape(replicas, -1, lane)], axis=1)
    rest_part = lax.psum_scatter(rest_term, "rep", scatter_dimension=0, tiled=False)
    ff_full = columns_home(ff_part)
    grad_attn_in = scatter_sum(dot_bt(grad_qkv, w_qkv))
    grad_norm_one = norm_back(grad_attn_in, normed_one, scale_one, gain_one)
    input_grad = (grad_hidden + grad_norm_one).astype(BF16)
    activ, grad_attn_in = lax.optimization_barrier((activ, grad_attn_in))
    last_sum = scatter_sum(dot(activ, w_down))
    output = (hidden_one + last_sum).astype(BF16)
    rest_part, last_sum = lax.optimization_barrier((rest_part, last_sum))
    small_home = lax.all_to_all(
        rest_part[:small_rows].reshape(groups, piece, qkv_cols),
        "fsdp", split_axis=0, concat_axis=0, tiled=True,
    ).reshape(small_rows, lane)
    down_full = replica_gather(down_part)
    rest_full = replica_gather(jnp.concatenate([small_home, rest_part[small_rows:]]))
    small_full = rest_full[:, :small_rows].reshape(replicas, groups, piece, qkv_cols)
    out_full = rest_full[:, small_rows:]

    gate_share, up_share = place_columns(ff_full, (ff_cols, ff_cols), (1, 1))
    query_share, key_share, value_share = place_columns(
        small_full, (q_cols, kv_cols, kv_cols), (1, spread, spread)
    )
    gain_terms = (
        gain_column(w_qkv, qkv_term, gain_one),
        gain_column(gate_cols, ff_term[:, :ff_cols], gain_two)
        + gain_column(up_cols, ff_term[:, ff_cols:], gain_two),
        head_terms[0],
        head_terms[1],
    )
    gain_terms, _ = lax.optimization_barrier((jnp.concatenate(gain_terms), last_sum))
    gain_sums = lax.psum(gain_terms, ("rep", "fsdp"))

    def own(first, length):
        return lax.dynamic_slice(gain_sums, (first + device * length,), (length,))

    return (
        output,
        input_grad,
        own(0, shard),
        query_share,
        key_share,
        value_share,
        own(2 * width, head_part),
        own(2 * width + HEAD_SIZE, head_part),
        out_full.reshape(w_out.shape).astype(F32),
        own(width, shard),
        gate_share,
        up_share,
        down_full.reshape(w_down.shape).astype(F32),
    )


def solution(mesh):
    rows = P(("rep", "fsdp"), None)
    vec = P("fsdp")
    mat = P("fsdp", None)
    return jax.shard_map(
        on_device,
        mesh=mesh,
        in_specs=(
            rows,
            rows,
            P("rep", None, None),
            P("rep", None),
            P("rep", "fsdp"),
            vec,
            mat,
            mat,
            mat,
            vec,
            vec,
            mat,
            vec,
            mat,
            mat,
            mat,
        ),
        out_specs=(rows, rows, vec, mat, mat, mat, vec, vec, mat, vec, mat, mat, mat),
        check_vma=False,
    )
```

```python
import functools
import math

import jax
import jax.numpy as jnp
from jax import lax
from jax.experimental import pallas as pl
from jax.experimental.pallas import tpu as pltpu
from jax.sharding import PartitionSpec as P


QUERY_HEADS = 16
KEY_VALUE_HEADS = 8
HEAD_SIZE = 128
SLOT_LENGTH = 288

EPSILON = 1e-06
ROPE_BASE = 1000000.0
NEG_LARGE = -1e30

F32 = jnp.float32
BF16 = jnp.bfloat16


def rms_scale(values):
    return lax.rsqrt(jnp.mean(values * values, axis=-1, keepdims=True) + EPSILON)


def dot(left, right):
    return jnp.dot(left, right, preferred_element_type=F32)


def dot_bt(left, right):
    return lax.dot_general(left, right, (((1,), (1,)), ((), ())), preferred_element_type=F32)


def dot_at(left, right):
    return lax.dot_general(left, right, (((0,), (0,)), ((), ())), preferred_element_type=F32)


def norm_back(grad_normed, unit_rows, scale_rows, gain_rows):
    scaled = grad_normed * gain_rows
    return scale_rows * (
        scaled - unit_rows * jnp.mean(scaled * unit_rows, axis=-1, keepdims=True)
    )


def partners(me):
    core, x_bit, y_bit = lax.rem(me, 2), lax.rem(me // 2, 2), me // 4
    along_x = me + 2 - 4 * x_bit
    along_y = me + 4 - 8 * y_bit
    return me + 1 - 2 * core, along_x, along_y, along_x + 4 - 8 * y_bit


def greet(devices):
    barrier = pltpu.get_barrier_semaphore()
    for device in devices:
        pl.semaphore_signal(
            barrier, inc=1, device_id={"fsdp": device}, device_id_type=pl.DeviceIdType.MESH
        )
    pl.semaphore_wait(barrier, len(devices))


def send(src, dst, send_sem, recv_sem, device):
    made = pltpu.make_async_remote_copy(
        src_ref=src,
        dst_ref=dst,
        send_sem=send_sem,
        recv_sem=recv_sem,
        device_id={"fsdp": device},
        device_id_type=pl.DeviceIdType.MESH,
    )
    made.start()
    return made


def exchange_rows(own, out, sends, recvs, local, between=None):
    me = lax.axis_index("fsdp")
    sib, along_x, along_y, across = partners(me)
    half = own.shape[1] // 2
    left, right = pl.ds(0, half), pl.ds(half, half)

    def copy(src, dst, slot, device):
        return send(src, dst, sends.at[slot], recvs.at[slot], device)

    mine = pltpu.make_async_copy(own, out.at[me], local)
    copies = [
        copy(own.at[:, left], out.at[me, :, left], 0, along_x),
        copy(own.at[:, right], out.at[me, :, right], 1, along_y),
        copy(own.at[:, right], out.at[me, :, right], 2, along_x),
        copy(own.at[:, left], out.at[me, :, left], 3, along_y),
        copy(own, out.at[me], 4, sib),
    ]
    mine.start()
    copies[0].wait_recv()
    copies.append(copy(out.at[along_x, :, left], out.at[along_x, :, left], 5, along_y))
    copies[1].wait_recv()
    copies.append(copy(out.at[along_y, :, right], out.at[along_y, :, right], 6, along_x))
    if between:
        between()
    copies[2].wait_recv()
    copies.append(copy(out.at[along_x], out.at[along_x], 7, sib))
    copies[3].wait_recv()
    copies.append(copy(out.at[along_y], out.at[along_y], 8, sib))
    copies[5].wait_recv()
    copies[6].wait_recv()
    copies.append(copy(out.at[across], out.at[across], 9, sib))
    for slot in (4, 7, 8, 9):
        copies[slot].wait_recv()
    mine.wait()
    for made in copies:
        made.wait_send()


def gather_kernel(own, out, sends, recvs, local):
    greet(partners(lax.axis_index("fsdp"))[:3])
    exchange_rows(own, out, sends, recvs, local)


def gather_rows(values, ident):
    rows, cols = values.shape
    return pl.pallas_call(
        gather_kernel,
        out_shape=jax.ShapeDtypeStruct((8, rows, cols), values.dtype),
        in_specs=[pl.BlockSpec(memory_space=pltpu.VMEM)],
        out_specs=pl.BlockSpec(memory_space=pl.ANY),
        scratch_shapes=[
            pltpu.SemaphoreType.DMA((10,)),
            pltpu.SemaphoreType.DMA((10,)),
            pltpu.SemaphoreType.DMA,
        ],
        compiler_params=pltpu.CompilerParams(collective_id=ident, has_side_effects=True),
        cost_estimate=pl.CostEstimate(
            flops=0, bytes_accessed=rows * cols * 180, transcendentals=0
        ),
        name="gather_rows",
    )(values).reshape(8 * rows, cols)


def flipped(me, flip):
    bits = (lax.rem(me, 2), lax.rem(me // 2, 2), me // 4)
    bits = [1 - bit if flip >> place & 1 else bit for place, bit in enumerate(bits)]
    return bits[0] + 2 * bits[1] + 4 * bits[2]


class Columns:
    def __init__(self, weights, taken, out, staged, sends, recvs, local):
        self.me = lax.axis_index("fsdp")
        self.weights, self.taken, self.out, self.staged = weights, taken, out, staged
        self.sends, self.recvs, self.local = sends, recvs, local
        self.peers = [(flip - 1, flipped(self.me, flip)) for flip in (6, 2, 4, 7, 3, 5, 1)]
        self.cuts = []
        at = 0
        for weight in weights:
            cols = weight.shape[1] // 8
            self.cuts.append(slice(at, at + cols))
            at += cols
        self.copies = []

    def source(self, index, device):
        cols = self.weights[index].shape[1] // 8
        return self.weights[index].at[
            self.taken, pl.ds(pl.multiple_of(device * cols, cols), cols)
        ]

    def stage(self):
        self.staging = [
            pltpu.make_async_copy(
                self.source(index, self.me), self.staged.at[:, cut], self.local.at[index]
            )
            for index, cut in enumerate(self.cuts)
        ]
        for made in self.staging:
            made.start()

    def send(self):
        for slot, device in self.peers:
            for index, cut in enumerate(self.cuts):
                self.copies.append(
                    send(
                        self.source(index, device),
                        self.out.at[self.me, :, cut],
                        self.sends.at[slot, index],
                        self.recvs.at[slot, index],
                        device,
                    )
                )

    def finish(self):
        for made in self.staging:
            made.wait()
        home = pltpu.make_async_copy(self.staged, self.out.at[self.me], self.local.at[0])
        home.start()
        for made in self.copies:
            made.wait_recv()
        for made in self.copies:
            made.wait_send()
        home.wait()


def columns_kernel(w_gate, w_up, *refs):
    piece = refs[0].shape[1]
    taken = pl.ds(pl.multiple_of(lax.axis_index("rep") * piece, piece), piece)
    parts = [
        Columns((weight,), taken, refs[index], *refs[2 + 4 * index : 6 + 4 * index])
        for index, weight in enumerate((w_gate, w_up))
    ]
    for columns in parts:
        columns.stage()
    greet([device for _, device in parts[0].peers])
    for columns in parts:
        columns.send()
    for columns in parts:
        columns.finish()


def start_kernel(
    own, w_query, w_key, w_value, out, w_qkv,
    staged, sends, recvs, local, w_sends, w_recvs, w_local,
):
    columns = Columns(
        (w_query, w_key, w_value), slice(None), w_qkv, staged, w_sends, w_recvs, w_local
    )
    columns.stage()
    greet([device for _, device in columns.peers])
    exchange_rows(own, out, sends, recvs, local, columns.send)
    columns.finish()


def columns_specs(weights, rows):
    cols = sum(w.shape[1] for w in weights) // 8
    count = len(weights)
    scratch = [
        pltpu.VMEM((rows, cols), BF16),
        pltpu.SemaphoreType.DMA((7, count)),
        pltpu.SemaphoreType.DMA((7, count)),
        pltpu.SemaphoreType.DMA((count,)),
    ]
    return jax.ShapeDtypeStruct((8, rows, cols), BF16), scratch


def send_columns(weights, rows, ident):
    specs = [columns_specs((weight,), rows) for weight in weights]
    anywhere = pl.BlockSpec(memory_space=pl.ANY)
    return pl.pallas_call(
        columns_kernel,
        out_shape=[shape for shape, _ in specs],
        in_specs=[anywhere] * len(weights),
        out_specs=[anywhere] * len(weights),
        scratch_shapes=sum([scratch for _, scratch in specs], []),
        compiler_params=pltpu.CompilerParams(collective_id=ident, has_side_effects=True),
        cost_estimate=pl.CostEstimate(
            flops=0, bytes_accessed=rows * weights[0].shape[1] * 120, transcendentals=0
        ),
        name="send_columns",
    )(*weights)


def width_of(shape):
    return shape.shape[-1]


def start(values, weights, ident):
    rows, cols = values.shape
    shape, scratch = columns_specs(weights, weights[0].shape[0])
    anywhere = pl.BlockSpec(memory_space=pl.ANY)
    got, w_qkv = pl.pallas_call(
        start_kernel,
        out_shape=(jax.ShapeDtypeStruct((8, rows, cols), values.dtype), shape),
        in_specs=[pl.BlockSpec(memory_space=pltpu.VMEM)] + [anywhere] * len(weights),
        out_specs=(anywhere,) * 2,
        scratch_shapes=[
            scratch[0],
            pltpu.SemaphoreType.DMA((10,)),
            pltpu.SemaphoreType.DMA((10,)),
            pltpu.SemaphoreType.DMA,
        ]
        + scratch[1:],
        compiler_params=pltpu.CompilerParams(collective_id=ident, has_side_effects=True),
        cost_estimate=pl.CostEstimate(
            flops=0, bytes_accessed=rows * cols * 300, transcendentals=0
        ),
        name="start",
    )(values, *weights)
    return got, w_qkv.reshape(-1, width_of(shape))


def scatter_kernel(parts, out, mine, other, first, second, send, recv, local):
    me = lax.axis_index("fsdp")
    sib, along_x, along_y, across = partners(me)
    rows, cols = out.shape
    half = cols // 2
    left, right = pl.ds(0, half), pl.ds(half, half)
    order = (across, along_x, along_y, me)
    loads = []
    for step, device in enumerate(order):
        load = pltpu.make_async_copy(parts.at[device], mine.at[step], local.at[step])
        load.start()
        loads.append(load)
    greet((sib, along_x, along_y))

    def copy(src, dst, slot, device):
        made = pltpu.make_async_remote_copy(
            src_ref=src,
            dst_ref=dst,
            send_sem=send.at[slot],
            recv_sem=recv.at[slot],
            device_id={"fsdp": device},
            device_id_type=pl.DeviceIdType.MESH,
        )
        made.start()
        return made

    copies = [
        copy(parts.at[device + sib - me], other.at[step], step, sib)
        for step, device in enumerate(order)
    ]

    def add(into, term, step_rows=16):
        @pl.loop(0, rows // step_rows)
        def _(index):
            at = pl.ds(pl.multiple_of(index * step_rows, step_rows), step_rows)
            into[at, :] = (into[at, :].astype(F32) + term[at, :].astype(F32)).astype(into.dtype)

    def own_chip(step):
        loads[step].wait()
        copies[step].wait_recv()
        add(mine.at[step], other.at[step])

    own_chip(0)
    copies.append(copy(mine.at[0, :, left], first.at[0], 4, along_x))
    copies.append(copy(mine.at[0, :, right], first.at[1], 5, along_y))
    own_chip(1)
    copies.append(copy(mine.at[1, :, left], first.at[2], 6, along_x))
    own_chip(2)
    copies.append(copy(mine.at[2, :, right], first.at[3], 7, along_y))
    own_chip(3)
    copies[4].wait_recv()
    add(mine.at[2, :, left], first.at[0])
    copies.append(copy(mine.at[2, :, left], second.at[0], 8, along_y))
    copies[5].wait_recv()
    add(mine.at[1, :, right], first.at[1])
    copies.append(copy(mine.at[1, :, right], second.at[1], 9, along_x))
    copies[6].wait_recv()
    copies[7].wait_recv()
    copies[8].wait_recv()
    copies[9].wait_recv()

    @pl.loop(0, rows // 16)
    def _(index):
        at = pl.ds(pl.multiple_of(index * 16, 16), 16)
        for side, cut in enumerate((left, right)):
            out[at, cut] = (
                mine[3, at, cut].astype(F32)
                + first[2 + side, at, :].astype(F32)
                + second[side, at, :].astype(F32)
            )

    for made in copies:
        made.wait_send()


def scatter_rows(values, ident):
    rows, cols = values.shape[0] // 8, values.shape[1]
    return pl.pallas_call(
        scatter_kernel,
        out_shape=jax.ShapeDtypeStruct((rows, cols), F32),
        in_specs=[pl.BlockSpec(memory_space=pl.ANY)],
        out_specs=pl.BlockSpec(memory_space=pltpu.VMEM),
        scratch_shapes=[
            pltpu.VMEM((4, rows, cols), BF16),
            pltpu.VMEM((4, rows, cols), BF16),
            pltpu.VMEM((4, rows, cols // 2), BF16),
            pltpu.VMEM((2, rows, cols // 2), BF16),
            pltpu.SemaphoreType.DMA((10,)),
            pltpu.SemaphoreType.DMA((10,)),
            pltpu.SemaphoreType.DMA((4,)),
        ],
        compiler_params=pltpu.CompilerParams(collective_id=ident, has_side_effects=True),
        cost_estimate=pl.CostEstimate(
            flops=0, bytes_accessed=rows * cols * 200, transcendentals=0
        ),
        name="scatter_rows",
    )(values.astype(BF16).reshape(8, rows, cols))


def place_kernel(widths, shared, got, *outs):
    at = 0
    for width, share, out in zip(widths, shared, outs):
        for place in range(got.shape[0] // share):
            total = got[place * share, :, at : at + width].astype(F32)
            for source in range(place * share + 1, (place + 1) * share):
                total = total + got[source, :, at : at + width].astype(F32)
            out[:, place * width : (place + 1) * width] = total
        at += width


def place_columns(full, widths, shared):
    replicas, groups, rows, cols = full.shape
    return pl.pallas_call(
        functools.partial(place_kernel, widths, shared),
        out_shape=[
            jax.ShapeDtypeStruct((replicas * rows, groups // share * width), F32)
            for width, share in zip(widths, shared)
        ],
        grid=(replicas,),
        in_specs=[pl.BlockSpec((None, groups, rows, cols), lambda i: (i, 0, 0, 0))],
        out_specs=[
            pl.BlockSpec((rows, groups // share * width), lambda i: (i, 0))
            for width, share in zip(widths, shared)
        ],
        cost_estimate=pl.CostEstimate(flops=0, bytes_accessed=full.size * 6, transcendentals=0),
        name="place_columns",
    )(full)


class Deal:
    def __init__(self, starts, places, counts, in_rows, cap):
        self.starts, self.places, self.counts = starts, places, counts
        self.in_rows = in_rows
        self.window = (cap + 14) // 8 * 8

    def sources(self, run):
        for source in range(self.starts.shape[0]):
            yield (
                source * self.in_rows + self.starts[source, run],
                self.places[source, run],
                self.counts[source, run],
            )

    def move(self, src, dst, src_at, dst_at, count):
        window = self.window
        src_base = jnp.minimum(src_at // 8 * 8, src.shape[0] - window)
        dst_base = jnp.minimum(dst_at // 8 * 8, dst.shape[0] - window)
        lead = dst_at - dst_base
        shift = lax.rem(lead - (src_at - src_base) + window, window)
        rows = src[pl.ds(pl.multiple_of(src_base, 8), window), :]
        rows = pltpu.roll(rows, shift, 0)
        into = pl.ds(pl.multiple_of(dst_base, 8), window)
        row = lax.broadcasted_iota(jnp.int32, rows.shape, 0)
        keep = (row >= lead) & (row < lead + count)
        dst[into, :] = jnp.where(keep, rows, dst[into, :])

    def load(self, packed, slot, run):
        for start, place, count in self.sources(run):
            self.move(packed, slot, start, place, count)

    def store(self, packed, slot, run):
        for start, place, count in self.sources(run):
            self.move(slot, packed, place, start, count)

    def length(self, run):
        total = 0
        for source in range(self.starts.shape[0]):
            total = total + self.counts[source, run]
        return total


KEY_SPAN = 384
BLOCKS = ((0, 128, 128), (128, 256, 256), (256, 288, KEY_SPAN))


def rotate(values, cosine, sine):
    return values * cosine + pltpu.roll(values, HEAD_SIZE // 2, 1) * sine


def unrotate(values, cosine, sine):
    return values * cosine + pltpu.roll(values * sine, HEAD_SIZE // 2, 1)


def block_probs(query, key, first, last, span, length):
    scores = dot_bt(query[first:last], key[:span]) * HEAD_SIZE ** (-0.5)
    row = first + lax.broadcasted_iota(jnp.int32, scores.shape, 0)
    column = lax.broadcasted_iota(jnp.int32, scores.shape, 1)
    scores = jnp.where((column <= row) & (column < length), scores, NEG_LARGE)
    exps = jnp.exp(scores - jnp.max(scores, axis=-1, keepdims=True))
    return exps * (1.0 / jnp.sum(exps, axis=-1, keepdims=True))


def attention_kernel(in_rows, cap, starts, places, counts, raw, gains, trig, out, slot, result, packed):
    deal = Deal(starts, places, counts, in_rows, cap)
    heads = out.shape[1] // HEAD_SIZE
    slot[...] = jnp.zeros_like(slot)
    length_rows = SLOT_LENGTH

    @pl.loop(0, starts.shape[0])
    def _(run):
        deal.load(raw, slot, run)
        length = deal.length(run)
        cosine, sine = trig[0], trig[1]
        key_at = heads * HEAD_SIZE
        key_raw = slot[:KEY_SPAN, key_at : key_at + HEAD_SIZE]
        key = rotate(key_raw * rms_scale(key_raw) * gains[1:2, :], cosine, sine).astype(BF16)
        value = slot[:KEY_SPAN, key_at + HEAD_SIZE :].astype(BF16)
        for head in range(heads):
            cut = slice(head * HEAD_SIZE, (head + 1) * HEAD_SIZE)
            query_raw = slot[:length_rows, cut]
            query = rotate(
                query_raw * rms_scale(query_raw) * gains[0:1, :],
                cosine[:length_rows],
                sine[:length_rows],
            ).astype(BF16)
            for first, last, span in BLOCKS:
                probs = block_probs(query, key, first, last, span, length)
                result[first:last, cut] = dot(probs.astype(BF16), value[:span])
        deal.store(packed, result, run)

    out[...] = packed[...].astype(BF16)


def attention_back_kernel(
    in_rows, cap, starts, places, counts, raw, grads, gains, trig, out, gain_out,
    slot, grad_slot, result, packed, key_sum, value_sum,
):
    deal = Deal(starts, places, counts, in_rows, cap)
    heads = grads.shape[1] // HEAD_SIZE
    slot[...] = jnp.zeros_like(slot)
    grad_slot[...] = jnp.zeros_like(grad_slot)
    gain_out[...] = jnp.zeros_like(gain_out)
    rows = SLOT_LENGTH

    def norm_and_store(grad, raw_rows, gain_row, cut, cosine, sine, gain_at):
        scale = rms_scale(raw_rows)
        unit = raw_rows * scale
        normed = unrotate(grad * HEAD_SIZE ** (-0.5), cosine, sine)
        gain_out[gain_at : gain_at + 1, :] += jnp.sum(normed * unit, axis=0, keepdims=True)
        result[:rows, cut] = norm_back(normed, unit, scale, gain_row)

    @pl.loop(0, starts.shape[0])
    def _(run):
        deal.load(raw, slot, run)
        deal.load(grads, grad_slot, run)
        length = deal.length(run)
        cosine, sine = trig[0], trig[1]
        key_at = heads * HEAD_SIZE
        key_raw = slot[:KEY_SPAN, key_at : key_at + HEAD_SIZE]
        key = rotate(key_raw * rms_scale(key_raw) * gains[1:2, :], cosine, sine).astype(BF16)
        value = slot[:KEY_SPAN, key_at + HEAD_SIZE :].astype(BF16)
        key_sum[...] = jnp.zeros_like(key_sum)
        value_sum[...] = jnp.zeros_like(value_sum)
        inside = lax.broadcasted_iota(jnp.int32, (rows, HEAD_SIZE), 0) < length
        for head in range(heads):
            cut = slice(head * HEAD_SIZE, (head + 1) * HEAD_SIZE)
            query_raw = slot[:rows, cut]
            query = rotate(
                query_raw * rms_scale(query_raw) * gains[0:1, :], cosine[:rows], sine[:rows]
            ).astype(BF16)
            grad_context = jnp.where(inside, grad_slot[:rows, cut], 0.0).astype(BF16)
            pieces = []
            for first, last, span in BLOCKS:
                probs = block_probs(query, key, first, last, span, length)
                grad_rows = grad_context[first:last]
                grad_probs = dot_bt(grad_rows, value[:span])
                value_sum[:span, :] += dot_at(probs.astype(BF16), grad_rows)
                inner = jnp.sum(grad_probs * probs, axis=-1, keepdims=True)
                grad_scores = (probs * (grad_probs - inner)).astype(BF16)
                pieces.append(dot(grad_scores, key[:span]))
                key_sum[:span, :] += dot_at(grad_scores, query[first:last])
            norm_and_store(
                jnp.concatenate(pieces), query_raw, gains[0:1, :], cut, cosine[:rows], sine[:rows], 0
            )
        norm_and_store(
            key_sum[:rows, :],
            key_raw[:rows],
            gains[1:2, :],
            slice(key_at, key_at + HEAD_SIZE),
            cosine[:rows],
            sine[:rows],
            1,
        )
        result[:rows, key_at + HEAD_SIZE :] = value_sum[:rows, :]
        deal.store(packed, result, run)

    out[...] = packed[...].astype(BF16)


def call_attention(kernel, tables, arrays, outs, scratch, in_rows, flops):
    cap = SLOT_LENGTH // tables[0].shape[0]
    vmem = pl.BlockSpec(memory_space=pltpu.VMEM)
    moved = sum(a.size * a.dtype.itemsize for a in arrays)
    return pl.pallas_call(
        functools.partial(kernel, in_rows, cap),
        out_shape=outs,
        in_specs=[pl.BlockSpec(memory_space=pltpu.SMEM)] * 3 + [vmem] * len(arrays),
        out_specs=jax.tree.map(lambda _: vmem, outs),
        scratch_shapes=[pltpu.VMEM(shape, F32) for shape in scratch],
        compiler_params=pltpu.CompilerParams(vmem_limit_bytes=48 << 20),
        cost_estimate=pl.CostEstimate(flops=flops, bytes_accessed=moved, transcendentals=1 << 20),
    )(*tables, *arrays)


def project_kernel(got, gain, weight, normed, raw):
    rows = got[: normed.shape[0], :].astype(F32)
    low = (rows * rms_scale(rows) * gain[...]).astype(BF16)
    normed[...] = low
    raw[...] = dot(low, weight[...])


def project(got, gain, weight, in_rows):
    groups, block, width = got.shape
    cols = weight.shape[1]
    return pl.pallas_call(
        project_kernel,
        out_shape=(
            jax.ShapeDtypeStruct((groups * in_rows, width), BF16),
            jax.ShapeDtypeStruct((groups * in_rows, cols), F32),
        ),
        grid=(groups,),
        in_specs=[
            pl.BlockSpec((None, block, width), lambda i: (i, 0, 0)),
            pl.BlockSpec((1, width), lambda i: (0, 0)),
            pl.BlockSpec((width, cols), lambda i: (0, 0)),
        ],
        out_specs=(
            pl.BlockSpec((in_rows, width), lambda i: (i, 0)),
            pl.BlockSpec((in_rows, cols), lambda i: (i, 0)),
        ),
        cost_estimate=pl.CostEstimate(
            flops=2 * groups * in_rows * width * cols,
            bytes_accessed=4 * got.size,
            transcendentals=0,
        ),
        name="project",
    )(got, gain[None], weight)


def feed_forward_kernel(rows, grads, w_gate, w_up, w_down, activ, grad_in):
    cols = activ.shape[1]
    step = cols // 3
    for at in range(0, cols, step):
        gate = dot(rows[...], w_gate[:, at : at + step])
        up = dot(rows[...], w_up[:, at : at + step])
        grad = dot_bt(grads[...], w_down[at : at + step, :])
        sigmoid = jax.nn.sigmoid(gate)
        silu = gate * sigmoid
        activ[:, at : at + step] = (silu * up).astype(BF16)
        grad_in[:, at : at + step] = (
            grad * up * sigmoid * (1.0 + gate * (1.0 - sigmoid))
        ).astype(BF16)
        grad_in[:, cols + at : cols + at + step] = (grad * silu).astype(BF16)


def feed_forward(rows, grads, w_gate, w_up, w_down, block):
    total, width = rows.shape
    cols = w_down.shape[0]
    row_spec = pl.BlockSpec((block, width), lambda i: (i, 0))
    return pl.pallas_call(
        feed_forward_kernel,
        out_shape=(
            jax.ShapeDtypeStruct((total, cols), BF16),
            jax.ShapeDtypeStruct((total, 2 * cols), BF16),
        ),
        grid=(total // block,),
        in_specs=[
            row_spec,
            row_spec,
            pl.BlockSpec(w_gate.shape, lambda i: (0, 0), pipeline_mode=pl.Buffered(1)),
            pl.BlockSpec(w_up.shape, lambda i: (0, 0), pipeline_mode=pl.Buffered(1)),
            pl.BlockSpec(w_down.shape, lambda i: (0, 0), pipeline_mode=pl.Buffered(1)),
        ],
        out_specs=(
            pl.BlockSpec((block, cols), lambda i: (i, 0)),
            pl.BlockSpec((block, 2 * cols), lambda i: (i, 0)),
        ),
        compiler_params=pltpu.CompilerParams(vmem_limit_bytes=48 << 20),
        cost_estimate=pl.CostEstimate(
            flops=6 * total * width * cols,
            bytes_accessed=4 * rows.size + 6 * w_down.size,
            transcendentals=total * cols,
        ),
        name="feed_forward",
    )(rows, grads, w_gate, w_up, w_down)


def input_grad_kernel(grads, w_gate, w_up, out):
    cols = w_gate.shape[1]
    gate, up = grads[:, :cols], grads[:, cols:]
    step = 512
    for at in range(0, out.shape[1], step):
        rows = slice(at, at + step)
        out[:, rows] = (dot_bt(gate, w_gate[rows, :]) + dot_bt(up, w_up[rows, :])).astype(BF16)


def input_grad_of(grads, w_gate, w_up, block):
    total, cols = grads.shape
    width = w_gate.shape[0]
    return pl.pallas_call(
        input_grad_kernel,
        out_shape=jax.ShapeDtypeStruct((total, width), BF16),
        grid=(total // block,),
        in_specs=[
            pl.BlockSpec((block, cols), lambda i: (i, 0)),
            pl.BlockSpec(w_gate.shape, lambda i: (0, 0), pipeline_mode=pl.Buffered(1)),
            pl.BlockSpec(w_up.shape, lambda i: (0, 0), pipeline_mode=pl.Buffered(1)),
        ],
        out_specs=pl.BlockSpec((block, width), lambda i: (i, 0)),
        compiler_params=pltpu.CompilerParams(vmem_limit_bytes=48 << 20),
        cost_estimate=pl.CostEstimate(
            flops=2 * total * width * cols,
            bytes_accessed=2 * grads.size + 2 * total * width + 4 * w_gate.size,
            transcendentals=0,
        ),
        name="input_grad",
    )(grads, w_gate, w_up)


def on_device(
    tokens,
    cotangent,
    counts,
    deal_order,
    seq_lengths,
    input_gain,
    w_query,
    key_projection,
    value_projection,
    query_gain,
    key_gain,
    w_out,
    mlp_gain,
    w_gate,
    w_up,
    w_down,
):
    groups = lax.axis_size("fsdp")
    replicas = lax.axis_size("rep")
    device = lax.axis_index("fsdp")
    in_rows, width = tokens.shape
    shard = width // groups
    heads = QUERY_HEADS // groups
    kv_heads = max(1, KEY_VALUE_HEADS // groups)
    spread = max(1, groups // KEY_VALUE_HEADS)
    q_cols, kv_cols = heads * HEAD_SIZE, kv_heads * HEAD_SIZE
    ff_cols = w_gate.shape[1] // groups

    def replica_gather(part):
        return lax.all_gather(part, "rep", axis=0, tiled=False)

    def gather(values):
        if groups != 8:
            return lax.all_gather(values, "fsdp", axis=0, tiled=True)
        return gather_rows(values, 0)

    def scatter_sum(values):
        if groups != 8:
            return lax.psum_scatter(
                values.astype(BF16), "fsdp", scatter_dimension=0, tiled=True
            ).astype(F32)
        return scatter_rows(values, 1)

    def replica_scatter(term, axis):
        return lax.psum_scatter(term, "rep", scatter_dimension=axis, tiled=True)

    def columns_home(part):
        part = lax.all_to_all(part, "fsdp", split_axis=0, concat_axis=0, tiled=True)
        return replica_gather(part)

    head_part = HEAD_SIZE // groups
    gain_row = jnp.concatenate([input_gain, mlp_gain, query_gain, key_gain])
    gain_row = jnp.pad(gain_row[None], ((0, 15), (0, width - gain_row.shape[0])))
    start_rows = jnp.concatenate([tokens, gain_row])
    if groups == 8:
        w_ff = send_columns((w_gate, w_up), shard // replicas, 3)
        start_rows, w_ff = lax.optimization_barrier((start_rows, w_ff))
        got, w_qkv = start(start_rows, (w_query, key_projection, value_projection), 2)
    else:
        got = gather(start_rows)
        kv_shape = (shard, KEY_VALUE_HEADS // kv_heads, kv_cols)
        keys = jnp.repeat(key_projection.reshape(kv_shape), spread, axis=1)
        values = jnp.repeat(value_projection.reshape(kv_shape), spread, axis=1)
        send_qkv = jnp.concatenate(
            [w_query.reshape(shard, groups, q_cols), keys, values], axis=2
        )
        w_qkv = lax.all_to_all(send_qkv, "fsdp", split_axis=1, concat_axis=0, tiled=True)
        w_qkv = w_qkv.reshape(width, q_cols + 2 * kv_cols)
        send_ff = jnp.concatenate(
            [w_gate.reshape(shard, groups, ff_cols), w_up.reshape(shard, groups, ff_cols)], axis=2
        )
        piece = shard // replicas
        send_ff = lax.dynamic_slice(
            send_ff, (lax.axis_index("rep") * piece, 0, 0), (piece, groups, 2 * ff_cols)
        )
        w_ff = lax.all_to_all(send_ff, "fsdp", split_axis=1, concat_axis=0, tiled=False)
        w_ff = w_ff.reshape(groups, piece, 2 * ff_cols)
        w_ff = (w_ff[:, :, :ff_cols], w_ff[:, :, ff_cols:])
    got = got.reshape(groups, in_rows + 16, width)
    got, cotangent_late = lax.optimization_barrier((got, cotangent))
    all_grads = lax.all_gather(cotangent_late, "fsdp", axis=0, tiled=True)

    def weight_columns(part):
        return lax.all_gather(part, "rep", axis=1, tiled=True).reshape(width, ff_cols)

    gate_cols = weight_columns(w_ff[0])
    up_cols = weight_columns(w_ff[1])
    gains = got[:, in_rows].astype(F32)
    gain_one = gains[:, :shard].reshape(width)
    gain_two = gains[:, shard : 2 * shard].reshape(width)
    gain_query = gains[:, 2 * shard : 2 * shard + head_part].reshape(HEAD_SIZE)
    gain_key = gains[:, 2 * shard + head_part : 2 * (shard + head_part)].reshape(HEAD_SIZE)

    table = counts[0]
    tables = (
        jnp.cumsum(table, axis=1) - table,
        jnp.cumsum(table, axis=0) - table,
        table,
    )

    resid = tokens.astype(F32)
    scale_one = rms_scale(resid)
    normed_one = resid * scale_one
    attention_input, raw = project(got, gain_one, w_qkv, in_rows)
    inverse = ROPE_BASE ** (-jnp.arange(0, HEAD_SIZE, 2, dtype=F32) / HEAD_SIZE)
    angles = jnp.arange(KEY_SPAN, dtype=F32)[:, None] * inverse
    cosine, sine = jnp.cos(angles), jnp.sin(angles)
    trig = jnp.stack(
        [jnp.concatenate([cosine, cosine], 1), jnp.concatenate([-sine, sine], 1)]
    )
    head_gains = jnp.stack([gain_query, gain_key])
    all_rows = groups * in_rows
    slot_rows = SLOT_LENGTH + HEAD_SIZE
    qkv_cols = q_cols + 2 * kv_cols
    context = call_attention(
        attention_kernel,
        tables,
        (raw, head_gains, trig),
        jax.ShapeDtypeStruct((all_rows, q_cols), BF16),
        ((slot_rows, qkv_cols), (slot_rows, q_cols), (all_rows, q_cols)),
        in_rows,
        4 * groups * heads * SLOT_LENGTH * SLOT_LENGTH * HEAD_SIZE,
    )
    hidden_one = resid + scatter_sum(dot(context, w_out))

    scale_two = rms_scale(hidden_one)
    normed_two = hidden_one * scale_two
    mlp_in = gather((normed_two * gain_two).astype(BF16))
    activ, grad_ff = feed_forward(mlp_in, all_grads, gate_cols, up_cols, w_down, 2 * in_rows)

    down_term = dot_at(activ, all_grads).astype(BF16)
    grad_ff, down_term = lax.optimization_barrier((grad_ff, down_term))
    down_part = replica_scatter(down_term, 0)
    ff_term = dot_at(mlp_in, grad_ff).astype(BF16)
    grad_ff, ff_term = lax.optimization_barrier((grad_ff, ff_term))
    ff_part = replica_scatter(ff_term.reshape(groups, shard, 2 * ff_cols), 1)
    grad_mlp_in = scatter_sum(input_grad_of(grad_ff, gate_cols, up_cols, 2 * in_rows))
    grad_norm_two = norm_back(grad_mlp_in, normed_two, scale_two, gain_two)
    grad_hidden = cotangent.astype(F32) + grad_norm_two

    all_hidden = gather(grad_hidden.astype(BF16))
    out_term = dot_at(context, all_hidden).astype(BF16)
    all_hidden, out_term = lax.optimization_barrier((all_hidden, out_term))
    grad_qkv, head_terms = call_attention(
        attention_back_kernel,
        tables,
        (raw, dot_bt(all_hidden, w_out), head_gains, trig),
        (
            jax.ShapeDtypeStruct((all_rows, qkv_cols), BF16),
            jax.ShapeDtypeStruct((8, HEAD_SIZE), F32),
        ),
        (
            (slot_rows, qkv_cols),
            (slot_rows, q_cols),
            (slot_rows, qkv_cols),
            (all_rows, qkv_cols),
            (KEY_SPAN, HEAD_SIZE),
            (KEY_SPAN, HEAD_SIZE),
        ),
        in_rows,
        10 * groups * heads * SLOT_LENGTH * SLOT_LENGTH * HEAD_SIZE,
    )
    qkv_term = dot_at(attention_input, grad_qkv).astype(BF16)

    def gain_column(weight, term, gain):
        return jnp.sum(weight.astype(F32) * term.astype(F32), axis=1) / gain

    small_term = qkv_term
    grad_qkv, small_term, ff_part = lax.optimization_barrier((grad_qkv, small_term, ff_part))
    piece = shard // replicas
    small_term = small_term.reshape(groups, replicas, piece, qkv_cols)
    lane = math.gcd(qkv_cols, width)
    small_term = jnp.swapaxes(small_term, 0, 1).reshape(replicas, -1, lane)
    small_rows = small_term.shape[1]
    rest_term = jnp.concatenate([small_term, out_term.reshape(replicas, -1, lane)], axis=1)
    rest_part = lax.psum_scatter(rest_term, "rep", scatter_dimension=0, tiled=False)
    ff_full = columns_home(ff_part)
    grad_attn_in = scatter_sum(dot_bt(grad_qkv, w_qkv))
    grad_norm_one = norm_back(grad_attn_in, normed_one, scale_one, gain_one)
    input_grad = (grad_hidden + grad_norm_one).astype(BF16)
    activ, grad_attn_in = lax.optimization_barrier((activ, grad_attn_in))
    last_sum = scatter_sum(dot(activ, w_down))
    output = (hidden_one + last_sum).astype(BF16)
    rest_part, last_sum = lax.optimization_barrier((rest_part, last_sum))
    small_home = lax.all_to_all(
        rest_part[:small_rows].reshape(groups, piece, qkv_cols),
        "fsdp", split_axis=0, concat_axis=0, tiled=True,
    ).reshape(small_rows, lane)
    down_full = replica_gather(down_part)
    rest_full = replica_gather(jnp.concatenate([small_home, rest_part[small_rows:]]))
    small_full = rest_full[:, :small_rows].reshape(replicas, groups, piece, qkv_cols)
    out_full = rest_full[:, small_rows:]

    gate_share, up_share = place_columns(ff_full, (ff_cols, ff_cols), (1, 1))
    query_share, key_share, value_share = place_columns(
        small_full, (q_cols, kv_cols, kv_cols), (1, spread, spread)
    )
    gain_terms = (
        gain_column(w_qkv, qkv_term, gain_one),
        gain_column(gate_cols, ff_term[:, :ff_cols], gain_two)
        + gain_column(up_cols, ff_term[:, ff_cols:], gain_two),
        head_terms[0],
        head_terms[1],
    )
    gain_terms, _ = lax.optimization_barrier((jnp.concatenate(gain_terms), last_sum))
    gain_sums = lax.psum(gain_terms, ("rep", "fsdp"))

    def own(first, length):
        return lax.dynamic_slice(gain_sums, (first + device * length,), (length,))

    return (
        output,
        input_grad,
        own(0, shard),
        query_share,
        key_share,
        value_share,
        own(2 * width, head_part),
        own(2 * width + HEAD_SIZE, head_part),
        out_full.reshape(w_out.shape).astype(F32),
        own(width, shard),
        gate_share,
        up_share,
        down_full.reshape(w_down.shape).astype(F32),
    )


def solution(mesh):
    rows = P(("rep", "fsdp"), None)
    vec = P("fsdp")
    mat = P("fsdp", None)
    return jax.shard_map(
        on_device,
        mesh=mesh,
        in_specs=(
            rows,
            rows,
            P("rep", None, None),
            P("rep", None),
            P("rep", "fsdp"),
            vec,
            mat,
            mat,
            mat,
            vec,
            vec,
            mat,
            vec,
            mat,
            mat,
            mat,
        ),
        out_specs=(rows, rows, vec, mat, mat, mat, vec, vec, mat, vec, mat, mat, mat),
        check_vma=False,
    )
```
